32 devices in a mesh: seq: 8 (over z, core), tp: 4 (over y, x).
Axes of the slice: x: 2, y: 2, z: 4, core: 2. Of those that a mesh axis runs over, the one named last changes fastest.
Arguments:
- queries: bfloat16 [8192, 4096], P(('seq', 'tp')), may hold values from -170 to 170, as said below
- keys: bfloat16 [8192, 512], P(('seq', 'tp')), may hold values from -6 to 6
- values: bfloat16 [8192, 512], P(('seq', 'tp')), may hold values from -6 to 6
- segments: int32 [8192], replicated, may hold values from 0 to 63, never falling along the last dimension, each value on 1 to 256 neighbouring positions
- out_weight: bfloat16 [4096, 4096], P('tp'), may hold values from -0.75 to 0.75
Outputs:
- mixed: bfloat16 [8192, 4096], P(('seq', 'tp'))
The draws below stay inside these ranges and needn't reach their ends.
Inputs may be any that keep to these rules, and one draw needn't show every extreme that they name: `segments`: document ids never fall along the positions; one document holds at most 256 positions. `queries`: independent entries.
All inputs are finite; a program needn't handle non-finite values.
Results may differ from the reference program's by a relative error of at most 0.014.
Values may be sent and summed in bfloat16 or wider, within the bound.
A program may use at most 64 MiB of HBM per device.

```python
import math
import jax
import jax.numpy as jnp
import numpy as np
from jax import lax

D = 4096
HQ = 32
KVH = 4
HD = 128
DOC = 256
TOKENS = 8192
N_TP = 4


def draw_queries(key, part):
    shape = (TOKENS, HQ * HD)
    base = jax.random.normal(jax.random.fold_in(key, 13), shape, jnp.float32)
    base = jnp.clip(base, -4.0, 4.0)
    return base.astype(jnp.bfloat16)


def block_scale(rng, extent, split, least, high):
    level = 1.0
    for axis_at, shards_of in split:
        steps = jax.random.uniform(jax.random.fold_in(jax.random.fold_in(rng, 6), axis_at), (shards_of,), jnp.float32, least / len(split), high / len(split))
        level = level * jnp.repeat(jnp.exp(steps), extent[axis_at] // shards_of).reshape((-1,) + (1,) * (len(extent) - 1 - axis_at))
    return level


def length_profile(number_of, total, limit, skew):
    weights = [(1 << 20) // math.isqrt(grade ** skew) + 1 for grade in range(2, number_of + 1)]
    surplus, given = total - limit - (number_of - 1), [1] * (number_of - 1)
    while surplus > 0:
        candidates = [i for i in range(number_of - 1) if given[i] < limit]
        mass, left = sum([weights[i] for i in candidates]), surplus
        for i in candidates:
            addition = min(limit - given[i], max(1, left * weights[i] // mass), surplus)
            given[i] = given[i] + addition
            surplus = surplus - addition
    return np.array([limit] + given)


def ragged(own_key, number_of, total, bound, lean):
    if number_of == 2:
        one = jax.random.randint(own_key, (), max(1, total - bound), min(bound, total - 1) + 1)
        return jnp.stack([one, total - one])
    lengths = jnp.asarray(length_profile(number_of, total, bound, lean), jnp.int32)
    couples = (number_of - 1) // 2
    source_of, receiver = lengths[1:1 + 2 * couples:2], lengths[2:2 + 2 * couples:2]
    room = jnp.minimum(source_of - 1, bound - receiver)
    shifted = jax.random.randint(jax.random.fold_in(own_key, 1), (couples,), 0, 1 << 20) % (room + 1)
    lengths = lengths.at[1:1 + 2 * couples:2].set(source_of - shifted).at[2:2 + 2 * couples:2].set(receiver + shifted)
    return lengths[jax.random.permutation(jax.random.fold_in(own_key, 2), number_of)]


def bell_draw(stream_key, dims, spread, limit, cuts=(), kind=jnp.bfloat16):
    loudness = block_scale(stream_key, dims, cuts, -0.22, 0.18) if cuts else 1.0
    drawn = jax.random.normal(stream_key, dims, jnp.float32) * spread * loudness
    return jnp.minimum(jnp.maximum(drawn, -limit), limit).astype(kind)


def setup_inputs(seed: int = 0) -> dict:
    key_of = jax.random.split(jax.random.key(seed), 6)
    queries = draw_queries(jax.random.fold_in(key_of[5], 71), 0)
    keys = bell_draw(key_of[1], (TOKENS, KVH * HD), 1.0, 6.0, ((0, 32),))
    values = bell_draw(key_of[2], (TOKENS, KVH * HD), 1.0, 6.0, ((0, 32),))
    segments = jnp.searchsorted(jnp.cumsum(ragged(key_of[3], TOKENS * 2 // DOC, TOKENS, DOC, 2)), jnp.arange(TOKENS), side="right").astype(jnp.int32)
    out_weight = bell_draw(key_of[4], (HQ * HD, D), (HD // 2) ** -0.5, 0.75, ((0, 4),))
    return {"queries": queries, "keys": keys, "values": values, "segments": segments, "out_weight": out_weight}


def reference(queries, keys, values, segments, out_weight):
    total = queries.shape[0]
    group_size = HQ // KVH
    tile_rows = DOC // 2
    width = DOC + tile_rows
    inverse_root = HD ** -0.5
    padded_keys = jnp.concatenate([jnp.zeros((DOC, KVH * HD), jnp.bfloat16), keys], 0)
    padded_values = jnp.concatenate([jnp.zeros((DOC, KVH * HD), jnp.bfloat16), values], 0)
    padded_seg = jnp.concatenate([jnp.full((DOC,), -1, jnp.int32), segments.astype(jnp.int32)], 0)

    def attend(index):
        start = (index * tile_rows).astype(jnp.int32)
        query_rows = lax.dynamic_slice_in_dim(queries, start, tile_rows, 0).astype(jnp.float32).reshape(tile_rows, KVH, group_size, HD)
        key_rows = lax.dynamic_slice_in_dim(padded_keys, start, width, 0).astype(jnp.float32).reshape(width, KVH, HD)
        value_rows = lax.dynamic_slice_in_dim(padded_values, start, width, 0).astype(jnp.float32).reshape(width, KVH, HD)
        key_seg = lax.dynamic_slice_in_dim(padded_seg, start, width, 0)
        query_seg = lax.dynamic_slice_in_dim(padded_seg, (start + DOC).astype(jnp.int32), tile_rows, 0)
        query_pos = start + jnp.arange(tile_rows, dtype=jnp.int32)
        key_pos = start - DOC + jnp.arange(width, dtype=jnp.int32)
        allowed = (key_pos[None, :] <= query_pos[:, None]) & (key_seg[None, :] == query_seg[:, None])
        scores = jnp.einsum("tkgd,skd->kgts", query_rows, key_rows) * inverse_root
        scores = jnp.where(allowed[None, None], scores, -1e30)
        top_score = jnp.max(scores, axis=-1, keepdims=True)
        weights = jnp.where(allowed[None, None], jnp.exp(scores - top_score), 0.0)
        denominator = jnp.sum(weights, axis=-1)
        rounded = lax.optimization_barrier(weights.astype(jnp.bfloat16)).astype(jnp.float32)
        output = jnp.einsum("kgts,skd->kgtd", rounded, value_rows) / denominator[..., None]
        output = jnp.transpose(output.astype(jnp.bfloat16), (2, 0, 1, 3))
        return output.reshape(tile_rows, HQ * HD)

    pieces = lax.map(attend, jnp.arange(total // tile_rows, dtype=jnp.int32))
    attended = pieces.reshape(total, HQ * HD)
    columns = HQ * HD // N_TP
    mixed = jnp.zeros((total, out_weight.shape[1]), jnp.float32)
    for owner in range(N_TP):
        partial_value = jnp.dot(attended[:, owner * columns:(owner + 1) * columns], out_weight[owner * columns:(owner + 1) * columns], preferred_element_type=jnp.float32)
        mixed = mixed + lax.optimization_barrier(partial_value.astype(jnp.bfloat16)).astype(jnp.float32)
    return mixed.astype(jnp.bfloat16)
```

```python
import functools

import jax
import jax.numpy as jnp
from jax import lax
from jax.experimental import pallas as pl
from jax.experimental.pallas import tpu as pltpu
from jax.sharding import PartitionSpec as P

KVH = 4
HD = 128
DOC = 256
TILE = DOC // 2


def from_behind(value, axis, steps):
    count = lax.axis_size(axis)
    first, last = (max(0, -steps), min(count, count - steps))
    return lax.ppermute(value, axis, [(source, source + steps) for source in range(first, last)])


def spread_heads(source, copies):
    if copies == 1:
        return source
    rows = source.shape[0]
    widened = jnp.repeat(source.reshape(rows, KVH, HD), copies, axis=1)
    return widened.reshape(rows, KVH * copies * HD)


def general_shards(queries, keys, values, segments, out_weight):
    tp_count = lax.axis_size("tp")
    copies = max(tp_count // KVH, 1)
    tile_rows = DOC // 2
    inverse_root = HD ** (-0.5)
    keys_wide = spread_heads(keys, copies)
    values_wide = spread_heads(values, copies)
    local_queries, local_keys, local_values = (
        lax.all_to_all(queries, "tp", split_axis=1, concat_axis=0, tiled=True),
        lax.all_to_all(keys_wide, "tp", split_axis=1, concat_axis=0, tiled=True),
        lax.all_to_all(values_wide, "tp", split_axis=1, concat_axis=0, tiled=True),
    )
    row_count = local_queries.shape[0]
    kv_local = local_keys.shape[1] // HD
    query_local = local_queries.shape[1] // HD
    local_group = query_local // kv_local
    tile_count = row_count // tile_rows
    first_row = lax.axis_index("seq") * row_count
    closing = jnp.stack([local_keys[row_count - DOC :], local_values[row_count - DOC :]])
    earlier = from_behind(closing, "seq", 1)
    key_ext = jnp.concatenate([earlier[0], local_keys], 0).reshape(row_count + DOC, kv_local, HD)
    value_ext = jnp.concatenate([earlier[1], local_values], 0).reshape(
        row_count + DOC, kv_local, HD
    )
    padded_seg = jnp.concatenate([jnp.full((DOC,), -1, jnp.int32), segments], 0)
    key_seg = lax.dynamic_slice_in_dim(padded_seg, first_row, row_count + DOC)
    query_seg = key_seg[DOC:].reshape(tile_count, tile_rows)
    key_pos = first_row - DOC + jnp.arange(row_count + DOC, dtype=jnp.int32)
    query_pos = (first_row + jnp.arange(row_count, dtype=jnp.int32)).reshape(tile_count, tile_rows)

    def windows(source):
        blocks = source.reshape((tile_count + 2, tile_rows) + source.shape[1:])
        return jnp.concatenate([blocks[:-2], blocks[1:-1], blocks[2:]], 1)

    key_win = windows(key_ext)
    value_win = windows(value_ext)
    pos_win = windows(key_pos)
    seg_win = windows(key_seg)
    query_tiles = local_queries.reshape(tile_count, tile_rows, kv_local, local_group, HD)
    allowed = (pos_win[:, None, :] <= query_pos[:, :, None]) & (
        seg_win[:, None, :] == query_seg[:, :, None]
    )
    allowed = allowed[:, None, None]
    scores = (
        jnp.einsum("ctkgd,cskd->ckgts", query_tiles, key_win, preferred_element_type=jnp.float32)
        * inverse_root
    )
    masked = jnp.where(allowed, scores, jnp.float32(-1e30))
    top_score = jnp.max(masked, axis=-1, keepdims=True)
    weights = jnp.where(allowed, jnp.exp(masked - top_score), jnp.float32(0.0))
    denominator = jnp.sum(weights, axis=-1)
    totals = jnp.einsum(
        "ckgts,cskd->ckgtd",
        weights.astype(jnp.bfloat16),
        value_win,
        preferred_element_type=jnp.float32,
    )
    attended = (totals / denominator[..., None]).astype(jnp.bfloat16)
    attended = jnp.transpose(attended, (0, 3, 1, 2, 4)).reshape(row_count, query_local * HD)
    return lax.psum_scatter(
        jnp.dot(attended, out_weight, preferred_element_type=jnp.float32).astype(jnp.bfloat16),
        "tp",
        scatter_dimension=0,
        tiled=True,
    )


PAIRS = 16
FIRST = 3
SECOND = 5
EARLY = 4


def kernel(
    n_seq,
    q_hbm,
    k_hbm,
    v_hbm,
    seg_hbm,
    w_hbm,
    out_ref,
    seg_ref,
    qbuf,
    kwin,
    vwin,
    w_ref,
    w_side,
    att,
    bias,
    part,
    own,
    arrived,
    local_sem,
    in_send,
    in_recv,
    before_send,
    before_recv,
    w_send,
    w_recv,
    out_send,
    out_recv,
):
    rows, width = qbuf.shape[1], qbuf.shape[2]
    pair_width = kwin.shape[2]
    group = width // pair_width
    depth, n_out = w_ref.shape
    pair_cols = n_out // PAIRS
    chunk = pair_cols // 2
    half = depth // 2
    s = lax.axis_index("seq")
    me = lax.axis_index("tp")
    x = me % 2
    y = me // 2
    xn = y * 2 + 1 - x
    yn = (1 - y) * 2 + x
    core = s % 2
    parity = (s // 2) % 2
    peer = s + 1 - 2 * core
    plane = s + 2 - 4 * parity
    blocks = (me, yn)
    f32, bf16 = jnp.float32, jnp.bfloat16

    def cols(index, size):
        return pl.ds(pl.multiple_of(index * size, size), size)

    late = pl.ds(rows, rows)
    early = pl.ds(0, rows)
    locals_ = [
        pltpu.make_async_copy(k_hbm.at[:, cols(y, pair_width)], kwin.at[0, late], local_sem.at[0]),
        pltpu.make_async_copy(v_hbm.at[:, cols(y, pair_width)], vwin.at[0, late], local_sem.at[1]),
        pltpu.make_async_copy(q_hbm.at[:, cols(y, width)], qbuf.at[0], local_sem.at[2]),
        pltpu.make_async_copy(w_hbm, w_ref, local_sem.at[3]),
        pltpu.make_async_copy(seg_hbm, seg_ref, local_sem.at[4]),
    ]
    for copy in locals_:
        copy.start()

    barrier = pltpu.get_barrier_semaphore()
    for target in ({"tp": xn}, {"tp": yn}, {"seq": peer}, {"seq": plane}):
        pl.semaphore_signal(barrier, inc=1, device_id=target)
    to_next = jnp.logical_and(x == 1, s < n_seq - 1)
    from_last = jnp.logical_and(x == 0, s > 0)

    @pl.when(to_next)
    def _():
        pl.semaphore_signal(barrier, inc=1, device_id={"seq": s + 1, "tp": xn})

    @pl.when(from_last)
    def _():
        pl.semaphore_signal(barrier, inc=1, device_id={"seq": s - 1, "tp": xn})

    pl.semaphore_wait(barrier, 4 + jnp.where(to_next, 1, 0) + jnp.where(from_last, 1, 0))

    def across(which):
        src, dst, size = (
            (k_hbm, kwin.at[1, late], pair_width),
            (v_hbm, vwin.at[1, late], pair_width),
        )[which]
        return pltpu.make_async_remote_copy(
            src_ref=src.at[:, cols(1 - y, size)],
            dst_ref=dst,
            send_sem=in_send.at[which],
            recv_sem=in_recv.at[which],
            device_id={"tp": yn},
        )

    def across_q(t, g):
        at = pl.ds(t * TILE, TILE)
        part_width = width // 2
        return pltpu.make_async_remote_copy(
            src_ref=q_hbm.at[at, cols((1 - y) * 2 + g, part_width)],
            dst_ref=qbuf.at[1, at, pl.ds(g * part_width, part_width)],
            send_sem=in_send.at[2 + 2 * t + g],
            recv_sem=in_recv.at[2 + 2 * t + g],
            device_id={"tp": yn},
        )

    def before(j, which, hop):
        win = (kwin, vwin)[which]
        src = (k_hbm, v_hbm)[which].at[:, cols(y, pair_width)] if j == 0 else win.at[1, late]
        slot = j + x * (1 - 2 * j)
        return pltpu.make_async_remote_copy(
            src_ref=src,
            dst_ref=win.at[slot, early],
            send_sem=before_send.at[which, j],
            recv_sem=before_recv.at[which, slot],
            device_id={"seq": lax.rem(s + hop, n_seq), "tp": xn},
        )

    def send_before(j):
        @pl.when(blocks[j] != 3)
        def _():
            before(j, 0, 0).start()
            before(j, 1, 0).start()

        @pl.when(jnp.logical_and(blocks[j] == 3, s < n_seq - 1))
        def _():
            before(j, 0, 1).start()
            before(j, 1, 1).start()

    def sent_before(j):
        @pl.when(jnp.logical_or(blocks[j] != 3, s < n_seq - 1))
        def _():
            before(j, 0, 0).wait_send()
            before(j, 1, 0).wait_send()

    def wait_before(j):
        @pl.when(jnp.logical_or(blocks[j] != 0, s > 0))
        def _():
            for which, win in enumerate((kwin, vwin)):
                pltpu.make_async_remote_copy(
                    src_ref=win.at[j, early],
                    dst_ref=win.at[j, early],
                    send_sem=before_send.at[which, j],
                    recv_sem=before_recv.at[which, j],
                    device_id={"tp": xn},
                ).wait_recv()

    mine = pl.ds(pl.multiple_of(core * half, half), half)

    def weight(i, stage):
        which = 1 - parity if stage == 3 else parity
        at = cols(2 * i + which, chunk)
        return pltpu.make_async_remote_copy(
            src_ref=(w_hbm if stage == 0 else w_side).at[mine, at],
            dst_ref=w_side.at[mine, at],
            send_sem=w_send.at[stage, i],
            recv_sem=w_recv.at[stage, i],
            device_id=({"tp": xn}, {"seq": plane}, {"seq": peer}, {"seq": peer})[stage],
        )

    def relay_direct(i):
        weight(i, 0).wait_recv()
        weight(i, 1).start()
        weight(i, 2).start()

    def relay_plane(i):
        weight(i, 1).wait_recv()
        weight(i, 3).start()

    across(0).start()
    across(1).start()
    tiles = rows // TILE
    for t in range(tiles):
        across_q(t, 0).start()
        across_q(t, 1).start()
    for i in range(FIRST):
        weight(i, 0).start()

    for j in range(2):

        @pl.when(jnp.logical_and(blocks[j] == 0, s == 0))
        def _():
            kwin[j, 0:rows] = jnp.zeros((rows, pair_width), bf16)
            vwin[j, 0:rows] = jnp.zeros((rows, pair_width), bf16)

    def send_halo(urgent):
        @pl.when(x == urgent)
        def _():
            send_before(0)

        @pl.when(x != urgent)
        def _():
            send_before(1)

    relay_direct(0)
    across(0).wait_recv()
    across(1).wait_recv()
    send_halo(1)
    for i in range(FIRST, SECOND):
        weight(i, 0).start()
    send_halo(0)

    @pl.loop(SECOND, PAIRS)
    def _(i):
        weight(i, 0).start()

    for copy in locals_:
        copy.wait()

    causal_q = lax.broadcasted_iota(jnp.int32, (TILE, TILE), 0)
    causal_k = lax.broadcasted_iota(jnp.int32, (TILE, TILE), 1)

    def attend(j, t, part_of):
        row = (s * 4 + blocks[j]) * tiles + t

        def seg_row(at):
            got = seg_ref[pl.ds(jnp.maximum(at, 0), 1), :]
            return jnp.broadcast_to(jnp.where(at >= 0, got, -1), (TILE, TILE))

        if part_of == 0:
            current = seg_row(row)
            down = jnp.transpose(current)
            low, zero = f32(-1e30), f32(0.0)
            bias[:, 0:TILE] = jnp.where(seg_row(row - 2) == down, zero, low)
            bias[:, TILE : 2 * TILE] = jnp.where(seg_row(row - 1) == down, zero, low)
            bias[:, 2 * TILE : 3 * TILE] = jnp.where(
                jnp.logical_and(current == down, causal_k <= causal_q), zero, low
            )
        here = pl.ds(t * TILE, TILE)
        window = pl.ds(t * TILE, 3 * TILE)
        heads = width // HD
        if j == 1:
            across_q(t, part_of).wait_recv()
        for h in range(part_of * (heads // 2), (part_of + 1) * (heads // 2)):
            span = slice(h * HD, (h + 1) * HD)
            kv = slice(h // group * HD, (h // group + 1) * HD)
            scores = lax.dot_general(
                qbuf[j, here, span],
                kwin[j, window, kv],
                (((1,), (1,)), ((), ())),
                preferred_element_type=f32,
            )
            scores = scores * (HD**-0.5) + bias[...]
            weights = jnp.exp(scores - jnp.max(scores, axis=-1, keepdims=True))
            denom = jnp.sum(weights, axis=-1, keepdims=True)
            total = jnp.dot(weights.astype(bf16), vwin[j, window, kv], preferred_element_type=f32)
            att[j, here, span] = (total / denom).astype(bf16)

    def product(j, at, here):
        return jnp.dot(
            att[j, here, cols(x, depth)], w_ref[:, at], preferred_element_type=f32
        ) + jnp.dot(att[j, here, cols(1 - x, depth)], w_side[:, at], preferred_element_type=f32)

    def outward(i, here, slot):
        at = cols(i, pair_cols)
        return pltpu.make_async_remote_copy(
            src_ref=part.at[here, at],
            dst_ref=arrived.at[here, at],
            send_sem=out_send.at[slot, i],
            recv_sem=out_recv.at[slot, i],
            device_id={"tp": yn},
        )

    every = pl.ds(0, rows)
    tile0, tile1 = pl.ds(0, TILE), pl.ds(TILE, TILE)

    def whole(i):
        weight(i, 2).wait_recv()
        weight(i, 3).wait_recv()

    def export(i, here, slot):
        part[here, cols(i, pair_cols)] = product(1, cols(i, pair_cols), here).astype(bf16)
        outward(i, here, slot).start()

    def keep(i):
        at = cols(i, 2 * pair_cols)
        own[:, at] = product(0, at, every)

    relay_direct(1)
    relay_plane(0)
    relay_direct(2)
    wait_before(1)
    attend(1, 0, 0)
    relay_plane(1)
    relay_plane(2)
    attend(1, 0, 1)
    relay_direct(3)
    for i in range(3):
        whole(i)
        export(i, tile0, 0)
    relay_direct(4)
    relay_plane(3)
    whole(3)
    export(3, tile0, 0)
    attend(1, 1, 0)
    relay_plane(4)
    relay_direct(5)
    attend(1, 1, 1)
    relay_direct(6)

    @pl.loop(0, EARLY)
    def _(i):
        export(i, tile1, 1)

    relay_plane(5)
    whole(4)
    export(4, every, 0)
    wait_before(0)
    attend(0, 0, 0)
    relay_direct(7)
    relay_plane(6)
    relay_direct(8)
    whole(5)
    export(5, every, 0)
    attend(0, 0, 1)
    relay_plane(7)
    relay_direct(9)
    whole(6)
    export(6, every, 0)
    attend(0, 1, 0)
    relay_plane(8)
    relay_direct(10)
    whole(7)
    export(7, every, 0)
    attend(0, 1, 1)
    relay_plane(9)
    relay_direct(11)

    @pl.loop(8, PAIRS)
    def _(i):
        whole(i)
        export(i, every, 0)

        @pl.when(i + 2 < PAIRS)
        def _():
            relay_plane(i + 2)

        @pl.when(i + 4 < PAIRS)
        def _():
            relay_direct(i + 4)

        keep(i - 8)

    @pl.loop(0, EARLY)
    def _(i):
        outward(i, tile0, 0).wait_recv()
        outward(i, tile1, 1).wait_recv()
        at = cols(i, pair_cols)
        out_ref[:, at] = (own[:, at] + arrived[:, at].astype(f32)).astype(bf16)

    @pl.loop(EARLY, PAIRS)
    def _(i):
        outward(i, every, 0).wait_recv()
        at = cols(i, pair_cols)
        out_ref[:, at] = (own[:, at] + arrived[:, at].astype(f32)).astype(bf16)

    across(0).wait_send()
    across(1).wait_send()
    for t in range(tiles):
        across_q(t, 0).wait_send()
        across_q(t, 1).wait_send()
    sent_before(0)
    sent_before(1)

    @pl.loop(0, PAIRS)
    def _(i):
        for stage in range(4):
            weight(i, stage).wait_send()

    @pl.loop(0, EARLY)
    def _(i):
        outward(i, tile0, 0).wait_send()
        outward(i, tile1, 1).wait_send()

    @pl.loop(EARLY, PAIRS)
    def _(i):
        outward(i, every, 0).wait_send()


def square_shards(n_seq, queries, keys, values, segments, out_weight):
    rows, n_q = queries.shape
    width = n_q // 2
    pair_width = keys.shape[1] // 2
    depth, n_out = out_weight.shape
    bf16 = jnp.bfloat16
    hbm = pl.BlockSpec(memory_space=pltpu.HBM)
    vmem = pl.BlockSpec(memory_space=pltpu.VMEM)
    dma = pltpu.SemaphoreType.DMA
    return pl.pallas_call(
        functools.partial(kernel, n_seq),
        out_shape=jax.ShapeDtypeStruct((rows, n_out), bf16),
        in_specs=[hbm, hbm, hbm, hbm, hbm],
        out_specs=vmem,
        scratch_shapes=[
            pltpu.VMEM((segments.shape[0] // TILE, TILE), jnp.int32),
            pltpu.VMEM((2, rows, width), bf16),
            pltpu.VMEM((2, 2 * rows, pair_width), bf16),
            pltpu.VMEM((2, 2 * rows, pair_width), bf16),
            pltpu.VMEM((depth, n_out), bf16),
            pltpu.VMEM((depth, n_out), bf16),
            pltpu.VMEM((2, rows, width), bf16),
            pltpu.VMEM((TILE, 3 * TILE), jnp.float32),
            pltpu.VMEM((rows, n_out), bf16),
            pltpu.VMEM((rows, n_out), jnp.float32),
            pltpu.VMEM((rows, n_out), bf16),
            dma((5,)),
            dma((2 + 2 * rows // TILE,)),
            dma((2 + 2 * rows // TILE,)),
            dma((2, 2)),
            dma((2, 2)),
            dma((4, PAIRS)),
            dma((4, PAIRS)),
            dma((2, PAIRS)),
            dma((2, PAIRS)),
        ],
        compiler_params=pltpu.CompilerParams(
            collective_id=0, has_side_effects=True, vmem_limit_bytes=50 * 1024 * 1024
        ),
    )(
        *(
            pltpu.with_memory_space_constraint(a, pltpu.HBM)
            for a in (queries, keys, values, segments.reshape(-1, TILE), out_weight)
        )
    )


def solution(mesh):
    placed = (
        P(("seq", "tp"), None),
        P(("seq", "tp"), None),
        P(("seq", "tp"), None),
        P(),
        P("tp", None),
    )
    n_seq, n_tp = mesh.shape["seq"], mesh.shape["tp"]

    def shards(queries, keys, values, segments, out_weight):
        one_head_each = keys.shape[1] == n_tp * HD
        fits = n_tp == 4 and n_seq % 4 == 0 and queries.shape[0] == DOC
        if fits and one_head_each:
            return square_shards(n_seq, queries, keys, values, segments, out_weight)
        return general_shards(queries, keys, values, segments, out_weight)

    return jax.shard_map(
        shards, mesh=mesh, in_specs=placed, out_specs=P(("seq", "tp"), None), check_vma=False
    )
```

```python
import functools

import jax
import jax.numpy as jnp
from jax import lax
from jax.experimental import pallas as pl
from jax.experimental.pallas import tpu as pltpu
from jax.sharding import PartitionSpec as P

KVH = 4
HD = 128
DOC = 256
TILE = DOC // 2


def from_behind(value, axis, steps):
    count = lax.axis_size(axis)
    first, last = (max(0, -steps), min(count, count - steps))
    return lax.ppermute(value, axis, [(source, source + steps) for source in range(first, last)])


def spread_heads(source, copies):
    if copies == 1:
        return source
    rows = source.shape[0]
    widened = jnp.repeat(source.reshape(rows, KVH, HD), copies, axis=1)
    return widened.reshape(rows, KVH * copies * HD)


def general_shards(queries, keys, values, segments, out_weight):
    tp_count = lax.axis_size("tp")
    copies = max(tp_count // KVH, 1)
    tile_rows = DOC // 2
    inverse_root = HD ** (-0.5)
    keys_wide = spread_heads(keys, copies)
    values_wide = spread_heads(values, copies)
    local_queries, local_keys, local_values = (
        lax.all_to_all(queries, "tp", split_axis=1, concat_axis=0, tiled=True),
        lax.all_to_all(keys_wide, "tp", split_axis=1, concat_axis=0, tiled=True),
        lax.all_to_all(values_wide, "tp", split_axis=1, concat_axis=0, tiled=True),
    )
    row_count = local_queries.shape[0]
    kv_local = local_keys.shape[1] // HD
    query_local = local_queries.shape[1] // HD
    local_group = query_local // kv_local
    tile_count = row_count // tile_rows
    first_row = lax.axis_index("seq") * row_count
    closing = jnp.stack([local_keys[row_count - DOC :], local_values[row_count - DOC :]])
    earlier = from_behind(closing, "seq", 1)
    key_ext = jnp.concatenate([earlier[0], local_keys], 0).reshape(row_count + DOC, kv_local, HD)
    value_ext = jnp.concatenate([earlier[1], local_values], 0).reshape(
        row_count + DOC, kv_local, HD
    )
    padded_seg = jnp.concatenate([jnp.full((DOC,), -1, jnp.int32), segments], 0)
    key_seg = lax.dynamic_slice_in_dim(padded_seg, first_row, row_count + DOC)
    query_seg = key_seg[DOC:].reshape(tile_count, tile_rows)
    key_pos = first_row - DOC + jnp.arange(row_count + DOC, dtype=jnp.int32)
    query_pos = (first_row + jnp.arange(row_count, dtype=jnp.int32)).reshape(tile_count, tile_rows)

    def windows(source):
        blocks = source.reshape((tile_count + 2, tile_rows) + source.shape[1:])
        return jnp.concatenate([blocks[:-2], blocks[1:-1], blocks[2:]], 1)

    key_win = windows(key_ext)
    value_win = windows(value_ext)
    pos_win = windows(key_pos)
    seg_win = windows(key_seg)
    query_tiles = local_queries.reshape(tile_count, tile_rows, kv_local, local_group, HD)
    allowed = (pos_win[:, None, :] <= query_pos[:, :, None]) & (
        seg_win[:, None, :] == query_seg[:, :, None]
    )
    allowed = allowed[:, None, None]
    scores = (
        jnp.einsum("ctkgd,cskd->ckgts", query_tiles, key_win, preferred_element_type=jnp.float32)
        * inverse_root
    )
    masked = jnp.where(allowed, scores, jnp.float32(-1e30))
    top_score = jnp.max(masked, axis=-1, keepdims=True)
    weights = jnp.where(allowed, jnp.exp(masked - top_score), jnp.float32(0.0))
    denominator = jnp.sum(weights, axis=-1)
    totals = jnp.einsum(
        "ckgts,cskd->ckgtd",
        weights.astype(jnp.bfloat16),
        value_win,
        preferred_element_type=jnp.float32,
    )
    attended = (totals / denominator[..., None]).astype(jnp.bfloat16)
    attended = jnp.transpose(attended, (0, 3, 1, 2, 4)).reshape(row_count, query_local * HD)
    return lax.psum_scatter(
        jnp.dot(attended, out_weight, preferred_element_type=jnp.float32).astype(jnp.bfloat16),
        "tp",
        scatter_dimension=0,
        tiled=True,
    )


PAIRS = 16
FIRST = 3
SECOND = 5
EARLY = 5


def kernel(
    n_seq,
    q_hbm,
    k_hbm,
    v_hbm,
    seg_hbm,
    w_hbm,
    out_ref,
    seg_ref,
    kv_out,
    qbuf,
    kwin,
    vwin,
    w_ref,
    w_side,
    att,
    bias,
    part,
    own,
    arrived,
    local_sem,
    in_send,
    in_recv,
    before_send,
    before_recv,
    w_send,
    w_recv,
    out_send,
    out_recv,
):
    rows, width = qbuf.shape[1], qbuf.shape[2]
    pair_width = kwin.shape[2]
    group = width // pair_width
    depth, n_out = w_ref.shape
    pair_cols = n_out // PAIRS
    chunk = pair_cols // 2
    half = depth // 2
    s = lax.axis_index("seq")
    me = lax.axis_index("tp")
    x = me % 2
    y = me // 2
    xn = y * 2 + 1 - x
    yn = (1 - y) * 2 + x
    core = s % 2
    parity = (s // 2) % 2
    peer = s + 1 - 2 * core
    plane = s + 2 - 4 * parity
    blocks = (me, yn)
    f32, bf16 = jnp.float32, jnp.bfloat16

    def cols(index, size):
        return pl.ds(pl.multiple_of(index * size, size), size)

    late = pl.ds(rows, rows)
    early = pl.ds(0, rows)
    early_ = [
        pltpu.make_async_copy(
            (k_hbm, v_hbm)[which].at[:, cols(1 - y, pair_width)],
            kv_out.at[which],
            local_sem.at[5 + which],
        )
        for which in range(2)
    ]
    for copy in early_:
        copy.start()
    locals_ = [
        pltpu.make_async_copy(k_hbm.at[:, cols(y, pair_width)], kwin.at[0, late], local_sem.at[0]),
        pltpu.make_async_copy(v_hbm.at[:, cols(y, pair_width)], vwin.at[0, late], local_sem.at[1]),
        pltpu.make_async_copy(q_hbm.at[:, cols(y, width)], qbuf.at[0], local_sem.at[2]),
        pltpu.make_async_copy(w_hbm, w_ref, local_sem.at[3]),
        pltpu.make_async_copy(seg_hbm, seg_ref, local_sem.at[4]),
    ]
    for copy in locals_:
        copy.start()

    barrier = pltpu.get_barrier_semaphore()
    for target in ({"tp": xn}, {"tp": yn}, {"seq": peer}, {"seq": plane}):
        pl.semaphore_signal(barrier, inc=1, device_id=target)
    to_next = jnp.logical_and(x == 1, s < n_seq - 1)
    from_last = jnp.logical_and(x == 0, s > 0)

    @pl.when(to_next)
    def _():
        pl.semaphore_signal(barrier, inc=1, device_id={"seq": s + 1, "tp": xn})

    @pl.when(from_last)
    def _():
        pl.semaphore_signal(barrier, inc=1, device_id={"seq": s - 1, "tp": xn})

    pl.semaphore_wait(barrier, 4 + jnp.where(to_next, 1, 0) + jnp.where(from_last, 1, 0))

    def across(which):
        return pltpu.make_async_remote_copy(
            src_ref=kv_out.at[which],
            dst_ref=(kwin, vwin)[which].at[1, late],
            send_sem=in_send.at[which],
            recv_sem=in_recv.at[which],
            device_id={"tp": yn},
        )

    def across_q(t, g):
        at = pl.ds(t * TILE, TILE)
        part_width = width // 2
        return pltpu.make_async_remote_copy(
            src_ref=q_hbm.at[at, cols((1 - y) * 2 + g, part_width)],
            dst_ref=qbuf.at[1, at, pl.ds(g * part_width, part_width)],
            send_sem=in_send.at[2 + 2 * t + g],
            recv_sem=in_recv.at[2 + 2 * t + g],
            device_id={"tp": yn},
        )

    def before(j, which, hop):
        win = (kwin, vwin)[which]
        src = (k_hbm, v_hbm)[which].at[:, cols(y, pair_width)] if j == 0 else win.at[1, late]
        slot = j + x * (1 - 2 * j)
        return pltpu.make_async_remote_copy(
            src_ref=src,
            dst_ref=win.at[slot, early],
            send_sem=before_send.at[which, j],
            recv_sem=before_recv.at[which, slot],
            device_id={"seq": lax.rem(s + hop, n_seq), "tp": xn},
        )

    def send_before(j):
        @pl.when(blocks[j] != 3)
        def _():
            before(j, 0, 0).start()
            before(j, 1, 0).start()

        @pl.when(jnp.logical_and(blocks[j] == 3, s < n_seq - 1))
        def _():
            before(j, 0, 1).start()
            before(j, 1, 1).start()

    def sent_before(j):
        @pl.when(jnp.logical_or(blocks[j] != 3, s < n_seq - 1))
        def _():
            before(j, 0, 0).wait_send()
            before(j, 1, 0).wait_send()

    def wait_before(j):
        @pl.when(jnp.logical_or(blocks[j] != 0, s > 0))
        def _():
            for which, win in enumerate((kwin, vwin)):
                pltpu.make_async_remote_copy(
                    src_ref=win.at[j, early],
                    dst_ref=win.at[j, early],
                    send_sem=before_send.at[which, j],
                    recv_sem=before_recv.at[which, j],
                    device_id={"tp": xn},
                ).wait_recv()

    mine = pl.ds(pl.multiple_of(core * half, half), half)
    theirs = pl.ds(pl.multiple_of((1 - core) * half, half), half)

    def weight(i, stage):
        which = 1 - parity if stage == 3 else parity
        at = cols(2 * i + which, chunk)
        return pltpu.make_async_remote_copy(
            src_ref=(w_hbm if stage == 0 else w_side).at[mine, at],
            dst_ref=w_side.at[mine, at],
            send_sem=w_send.at[stage],
            recv_sem=w_recv.at[min(stage, 2), i],
            device_id=({"tp": xn}, {"seq": plane}, {"seq": peer}, {"seq": peer})[stage],
        )

    def relay_direct(i):
        weight(i, 0).wait_recv()
        weight(i, 1).start()
        weight(i, 2).start()

    def relay_plane(i):
        weight(i, 1).wait_recv()
        weight(i, 3).start()

    for which in range(2):
        early_[which].wait()
        across(which).start()
    tiles = rows // TILE
    for t in range(tiles):
        across_q(t, 0).start()
        across_q(t, 1).start()
    for i in range(FIRST):
        weight(i, 0).start()

    for j in range(2):

        @pl.when(jnp.logical_and(blocks[j] == 0, s == 0))
        def _():
            kwin[j, 0:rows] = jnp.zeros((rows, pair_width), bf16)
            vwin[j, 0:rows] = jnp.zeros((rows, pair_width), bf16)

    def send_halo(urgent):
        @pl.when(x == urgent)
        def _():
            send_before(0)

        @pl.when(x != urgent)
        def _():
            send_before(1)

    relay_direct(0)
    across(0).wait_recv()
    across(1).wait_recv()
    send_halo(1)
    for i in range(FIRST, SECOND):
        weight(i, 0).start()
    send_halo(0)

    @pl.loop(SECOND, PAIRS)
    def _(i):
        weight(i, 0).start()

    for copy in locals_:
        copy.wait()

    causal_q = lax.broadcasted_iota(jnp.int32, (TILE, TILE), 0)
    causal_k = lax.broadcasted_iota(jnp.int32, (TILE, TILE), 1)

    def attend(j, t, quarter):
        row = (s * 4 + blocks[j]) * tiles + t

        def seg_row(at):
            got = seg_ref[pl.ds(jnp.maximum(at, 0), 1), :]
            return jnp.broadcast_to(jnp.where(at >= 0, got, -1), (TILE, TILE))

        if quarter == 0:
            current = seg_row(row)
            down = jnp.transpose(current)
            low, zero = f32(-1e30), f32(0.0)
            bias[:, 0:TILE] = jnp.where(seg_row(row - 2) == down, zero, low)
            bias[:, TILE : 2 * TILE] = jnp.where(seg_row(row - 1) == down, zero, low)
            bias[:, 2 * TILE : 3 * TILE] = jnp.where(
                jnp.logical_and(current == down, causal_k <= causal_q), zero, low
            )
        here = pl.ds(t * TILE, TILE)
        window = pl.ds(t * TILE, 3 * TILE)
        heads = width // HD
        if j == 1 and quarter % 2 == 0:
            across_q(t, quarter // 2).wait_recv()
        for h in range(quarter * (heads // 4), (quarter + 1) * (heads // 4)):
            span = slice(h * HD, (h + 1) * HD)
            kv = slice(h // group * HD, (h // group + 1) * HD)
            scores = lax.dot_general(
                qbuf[j, here, span],
                kwin[j, window, kv],
                (((1,), (1,)), ((), ())),
                preferred_element_type=f32,
            )
            scores = scores * (HD**-0.5) + bias[...]
            weights = jnp.exp(scores - jnp.max(scores, axis=-1, keepdims=True))
            denom = jnp.sum(weights, axis=-1, keepdims=True)
            total = jnp.dot(weights.astype(bf16), vwin[j, window, kv], preferred_element_type=f32)
            att[j, here, span] = (total / denom).astype(bf16)

    def product(j, at, here):
        return jnp.dot(
            att[j, here, cols(x, depth)], w_ref[:, at], preferred_element_type=f32
        ) + jnp.dot(att[j, here, cols(1 - x, depth)], w_side[:, at], preferred_element_type=f32)

    def outward(here, at, group):
        return pltpu.make_async_remote_copy(
            src_ref=part.at[here, at],
            dst_ref=arrived.at[here, at],
            send_sem=out_send.at[0],
            recv_sem=out_recv.at[group],
            device_id={"tp": yn},
        )

    every = pl.ds(0, rows)
    tile0, tile1 = pl.ds(0, TILE), pl.ds(TILE, TILE)

    def whole(i):
        held = w_side.at[theirs, cols(i, pair_cols)]
        pltpu.make_async_remote_copy(
            src_ref=held,
            dst_ref=held,
            send_sem=w_send.at[2],
            recv_sem=w_recv.at[2, i],
            device_id={"seq": peer},
        ).wait_recv()

    def export(i, here, group):
        at = cols(i, pair_cols)
        part[here, at] = product(1, at, here).astype(bf16)
        outward(here, at, group).start()

    def keep(i):
        at = cols(i, 2 * pair_cols)
        own[:, at] = product(0, at, every)

    relay_direct(1)
    relay_plane(0)
    relay_direct(2)
    relay_plane(1)
    wait_before(1)
    attend(1, 0, 0)
    attend(1, 0, 1)
    relay_plane(2)
    relay_direct(3)
    attend(1, 0, 2)
    attend(1, 0, 3)
    whole(0)
    export(0, tile0, 0)
    whole(1)
    export(1, tile0, 0)
    whole(2)
    export(2, tile0, 0)
    relay_direct(4)
    relay_plane(3)
    attend(1, 1, 0)
    whole(3)
    export(3, tile0, 0)
    attend(1, 1, 1)
    relay_plane(4)
    whole(4)
    export(4, tile0, 0)
    relay_direct(5)
    attend(1, 1, 2)
    attend(1, 1, 3)
    relay_direct(6)

    @pl.loop(0, EARLY)
    def _(i):
        export(i, tile1, 0)

    relay_direct(7)
    wait_before(0)
    attend(0, 0, 0)
    relay_plane(5)
    relay_direct(8)
    attend(0, 0, 1)
    relay_plane(6)
    whole(5)
    export(5, every, 0)
    relay_direct(9)
    relay_plane(7)
    whole(6)
    export(6, every, 0)
    attend(0, 0, 2)
    relay_direct(10)
    relay_plane(8)
    whole(7)
    export(7, every, 0)
    attend(0, 0, 3)
    relay_direct(11)
    relay_plane(9)
    whole(8)
    export(8, every, 0)
    attend(0, 1, 0)
    relay_direct(12)
    relay_plane(10)
    whole(9)
    export(9, every, 0)
    attend(0, 1, 1)
    relay_direct(13)
    relay_plane(11)
    whole(10)
    export(10, every, 0)
    attend(0, 1, 2)
    relay_direct(14)
    relay_plane(12)
    whole(11)
    export(11, every, 0)
    attend(0, 1, 3)
    relay_direct(15)
    relay_plane(13)
    whole(12)
    export(12, every, 0)
    keep(0)
    relay_plane(14)
    whole(13)
    export(13, every, 0)
    keep(1)
    relay_plane(15)
    whole(14)
    export(14, every, 1)
    keep(2)
    whole(15)
    export(15, every, 2)

    @pl.loop(3, 8)
    def _(i):
        keep(i)


    across(0).wait_send()
    across(1).wait_send()
    for t in range(tiles):
        across_q(t, 0).wait_send()
        across_q(t, 1).wait_send()
    sent_before(0)
    sent_before(1)

    for stage in range(4):
        sent = w_side.at[mine, pl.ds(0, n_out // 2)]
        pltpu.make_async_remote_copy(
            src_ref=sent,
            dst_ref=sent,
            send_sem=w_send.at[stage],
            recv_sem=w_recv.at[0, 0],
            device_id={"tp": xn},
        ).wait_send()

    def settle(at):
        out_ref[:, at] = (own[:, at] + arrived[:, at].astype(f32)).astype(bf16)

    outward(every, pl.ds(0, (PAIRS - 2) * pair_cols), 0).wait_recv()

    @pl.loop(0, PAIRS // 2 - 1)
    def _(i):
        settle(cols(i, 2 * pair_cols))

    for i in range(PAIRS - 2, PAIRS):
        at = cols(i, pair_cols)
        outward(every, at, i - PAIRS + 3).wait_recv()
        settle(at)
    outward(every, pl.ds(0, n_out), 0).wait_send()


def square_shards(n_seq, queries, keys, values, segments, out_weight):
    rows, n_q = queries.shape
    width = n_q // 2
    pair_width = keys.shape[1] // 2
    depth, n_out = out_weight.shape
    bf16 = jnp.bfloat16
    hbm = pl.BlockSpec(memory_space=pltpu.HBM)
    vmem = pl.BlockSpec(memory_space=pltpu.VMEM)
    dma = pltpu.SemaphoreType.DMA
    return pl.pallas_call(
        functools.partial(kernel, n_seq),
        out_shape=jax.ShapeDtypeStruct((rows, n_out), bf16),
        in_specs=[hbm, hbm, hbm, hbm, hbm],
        out_specs=vmem,
        scratch_shapes=[
            pltpu.VMEM((segments.shape[0] // TILE, TILE), jnp.int32),
            pltpu.VMEM((2, rows, pair_width), bf16),
            pltpu.VMEM((2, rows, width), bf16),
            pltpu.VMEM((2, 2 * rows, pair_width), bf16),
            pltpu.VMEM((2, 2 * rows, pair_width), bf16),
            pltpu.VMEM((depth, n_out), bf16),
            pltpu.VMEM((depth, n_out), bf16),
            pltpu.VMEM((2, rows, width), bf16),
            pltpu.VMEM((TILE, 3 * TILE), jnp.float32),
            pltpu.VMEM((rows, n_out), bf16),
            pltpu.VMEM((rows, n_out), jnp.float32),
            pltpu.VMEM((rows, n_out), bf16),
            dma((7,)),
            dma((2 + 2 * rows // TILE,)),
            dma((2 + 2 * rows // TILE,)),
            dma((2, 2)),
            dma((2, 2)),
            dma((4,)),
            dma((3, PAIRS)),
            dma((1,)),
            dma((3,)),
        ],
        compiler_params=pltpu.CompilerParams(
            collective_id=0, has_side_effects=True, vmem_limit_bytes=50 * 1024 * 1024
        ),
    )(
        *(
            pltpu.with_memory_space_constraint(a, pltpu.HBM)
            for a in (queries, keys, values, segments.reshape(-1, TILE), out_weight)
        )
    )


def solution(mesh):
    placed = (
        P(("seq", "tp"), None),
        P(("seq", "tp"), None),
        P(("seq", "tp"), None),
        P(),
        P("tp", None),
    )
    n_seq, n_tp = mesh.shape["seq"], mesh.shape["tp"]

    def shards(queries, keys, values, segments, out_weight):
        one_head_each = keys.shape[1] == n_tp * HD
        fits = n_tp == 4 and n_seq % 4 == 0 and queries.shape[0] == DOC
        if fits and one_head_each:
            return square_shards(n_seq, queries, keys, values, segments, out_weight)
        return general_shards(queries, keys, values, segments, out_weight)

    return jax.shard_map(
        shards, mesh=mesh, in_specs=placed, out_specs=P(("seq", "tp"), None), check_vma=False
    )
```

```python
import functools

import jax
import jax.numpy as jnp
from jax import lax
from jax.experimental import pallas as pl
from jax.experimental.pallas import tpu as pltpu
from jax.sharding import PartitionSpec as P

KVH = 4
HD = 128
DOC = 256
TILE = DOC // 2


def from_behind(value, axis, steps):
    count = lax.axis_size(axis)
    first, last = (max(0, -steps), min(count, count - steps))
    return lax.ppermute(value, axis, [(source, source + steps) for source in range(first, last)])


def spread_heads(source, copies):
    if copies == 1:
        return source
    rows = source.shape[0]
    widened = jnp.repeat(source.reshape(rows, KVH, HD), copies, axis=1)
    return widened.reshape(rows, KVH * copies * HD)


def general_shards(queries, keys, values, segments, out_weight):
    tp_count = lax.axis_size("tp")
    copies = max(tp_count // KVH, 1)
    tile_rows = DOC // 2
    inverse_root = HD ** (-0.5)
    keys_wide = spread_heads(keys, copies)
    values_wide = spread_heads(values, copies)
    local_queries, local_keys, local_values = (
        lax.all_to_all(queries, "tp", split_axis=1, concat_axis=0, tiled=True),
        lax.all_to_all(keys_wide, "tp", split_axis=1, concat_axis=0, tiled=True),
        lax.all_to_all(values_wide, "tp", split_axis=1, concat_axis=0, tiled=True),
    )
    row_count = local_queries.shape[0]
    kv_local = local_keys.shape[1] // HD
    query_local = local_queries.shape[1] // HD
    local_group = query_local // kv_local
    tile_count = row_count // tile_rows
    first_row = lax.axis_index("seq") * row_count
    closing = jnp.stack([local_keys[row_count - DOC :], local_values[row_count - DOC :]])
    earlier = from_behind(closing, "seq", 1)
    key_ext = jnp.concatenate([earlier[0], local_keys], 0).reshape(row_count + DOC, kv_local, HD)
    value_ext = jnp.concatenate([earlier[1], local_values], 0).reshape(
        row_count + DOC, kv_local, HD
    )
    padded_seg = jnp.concatenate([jnp.full((DOC,), -1, jnp.int32), segments], 0)
    key_seg = lax.dynamic_slice_in_dim(padded_seg, first_row, row_count + DOC)
    query_seg = key_seg[DOC:].reshape(tile_count, tile_rows)
    key_pos = first_row - DOC + jnp.arange(row_count + DOC, dtype=jnp.int32)
    query_pos = (first_row + jnp.arange(row_count, dtype=jnp.int32)).reshape(tile_count, tile_rows)

    def windows(source):
        blocks = source.reshape((tile_count + 2, tile_rows) + source.shape[1:])
        return jnp.concatenate([blocks[:-2], blocks[1:-1], blocks[2:]], 1)

    key_win = windows(key_ext)
    value_win = windows(value_ext)
    pos_win = windows(key_pos)
    seg_win = windows(key_seg)
    query_tiles = local_queries.reshape(tile_count, tile_rows, kv_local, local_group, HD)
    allowed = (pos_win[:, None, :] <= query_pos[:, :, None]) & (
        seg_win[:, None, :] == query_seg[:, :, None]
    )
    allowed = allowed[:, None, None]
    scores = (
        jnp.einsum("ctkgd,cskd->ckgts", query_tiles, key_win, preferred_element_type=jnp.float32)
        * inverse_root
    )
    masked = jnp.where(allowed, scores, jnp.float32(-1e30))
    top_score = jnp.max(masked, axis=-1, keepdims=True)
    weights = jnp.where(allowed, jnp.exp(masked - top_score), jnp.float32(0.0))
    denominator = jnp.sum(weights, axis=-1)
    totals = jnp.einsum(
        "ckgts,cskd->ckgtd",
        weights.astype(jnp.bfloat16),
        value_win,
        preferred_element_type=jnp.float32,
    )
    attended = (totals / denominator[..., None]).astype(jnp.bfloat16)
    attended = jnp.transpose(attended, (0, 3, 1, 2, 4)).reshape(row_count, query_local * HD)
    return lax.psum_scatter(
        jnp.dot(attended, out_weight, preferred_element_type=jnp.float32).astype(jnp.bfloat16),
        "tp",
        scatter_dimension=0,
        tiled=True,
    )


PAIRS = 16
FIRST = 3
SECOND = 5
EARLY = 5


def kernel(
    n_seq,
    q_hbm,
    k_hbm,
    v_hbm,
    seg_hbm,
    w_hbm,
    out_ref,
    seg_ref,
    kv_out,
    qbuf,
    kwin,
    vwin,
    w_ref,
    w_side,
    att,
    bias,
    part,
    own,
    arrived,
    local_sem,
    in_send,
    in_recv,
    before_send,
    before_recv,
    w_send,
    w_recv,
    out_send,
    out_recv,
    entered,
):
    rows, width = qbuf.shape[1], qbuf.shape[2]
    pair_width = kwin.shape[2]
    group = width // pair_width
    depth, n_out = w_ref.shape
    pair_cols = n_out // PAIRS
    chunk = pair_cols // 2
    half = depth // 2
    s = lax.axis_index("seq")
    me = lax.axis_index("tp")
    x = me % 2
    y = me // 2
    xn = y * 2 + 1 - x
    yn = (1 - y) * 2 + x
    core = s % 2
    parity = (s // 2) % 2
    peer = s + 1 - 2 * core
    plane = s + 2 - 4 * parity
    blocks = (me, yn)
    f32, bf16 = jnp.float32, jnp.bfloat16

    def cols(index, size):
        return pl.ds(pl.multiple_of(index * size, size), size)

    late = pl.ds(rows, rows)
    early = pl.ds(0, rows)
    early_ = [
        pltpu.make_async_copy(
            (k_hbm, v_hbm)[which].at[:, cols(1 - y, pair_width)],
            kv_out.at[which],
            local_sem.at[5 + which],
        )
        for which in range(2)
    ]
    for copy in early_:
        copy.start()
    locals_ = [
        pltpu.make_async_copy(k_hbm.at[:, cols(y, pair_width)], kwin.at[0, late], local_sem.at[0]),
        pltpu.make_async_copy(v_hbm.at[:, cols(y, pair_width)], vwin.at[0, late], local_sem.at[1]),
        pltpu.make_async_copy(q_hbm.at[:, cols(y, width)], qbuf.at[0], local_sem.at[2]),
        pltpu.make_async_copy(w_hbm, w_ref, local_sem.at[3]),
        pltpu.make_async_copy(seg_hbm, seg_ref, local_sem.at[4]),
    ]
    for copy in locals_:
        copy.start()

    barrier = pltpu.get_barrier_semaphore()
    for target in ({"tp": xn}, {"tp": yn}, {"seq": peer}, {"seq": plane}):
        pl.semaphore_signal(barrier, inc=1, device_id=target)
    ahead = jnp.logical_and(x == 1, s < n_seq - 1)
    behind = jnp.logical_and(x == 1, s > 0)
    above = jnp.logical_and(ahead, core == 1)
    below = jnp.logical_and(behind, core == 0)

    @pl.when(above)
    def _():
        pl.semaphore_signal(barrier, inc=1, device_id={"seq": s + 1})

    @pl.when(below)
    def _():
        pl.semaphore_signal(barrier, inc=1, device_id={"seq": s - 1})

    pl.semaphore_wait(barrier, 4 + jnp.where(above, 1, 0) + jnp.where(below, 1, 0))

    @pl.when(behind)
    def _():
        pl.semaphore_signal(entered, inc=1, device_id={"seq": s - 1})

    def across(which):
        return pltpu.make_async_remote_copy(
            src_ref=kv_out.at[which],
            dst_ref=(kwin, vwin)[which].at[1, late],
            send_sem=in_send.at[0],
            recv_sem=in_recv.at[which],
            device_id={"tp": yn},
        )

    def across_q(t, g):
        at = pl.ds(t * TILE, TILE)
        part_width = width // 2
        return pltpu.make_async_remote_copy(
            src_ref=q_hbm.at[at, cols((1 - y) * 2 + g, part_width)],
            dst_ref=qbuf.at[1, at, pl.ds(g * part_width, part_width)],
            send_sem=in_send.at[1],
            recv_sem=in_recv.at[2 + 2 * t + g],
            device_id={"tp": yn},
        )

    def before(j, which, hop):
        win = (kwin, vwin)[which]
        src = (k_hbm, v_hbm)[which].at[:, cols(y, pair_width)] if j == 0 else win.at[1, late]
        slot = j + x * (1 - 2 * j)
        return pltpu.make_async_remote_copy(
            src_ref=src,
            dst_ref=win.at[slot, early],
            send_sem=before_send.at[j],
            recv_sem=before_recv.at[which, slot],
            device_id={"seq": lax.rem(s + hop, n_seq), "tp": xn},
        )

    def send_before(j):
        @pl.when(blocks[j] != 3)
        def _():
            before(j, 0, 0).start()
            before(j, 1, 0).start()

        @pl.when(jnp.logical_and(blocks[j] == 3, s < n_seq - 1))
        def _():
            before(j, 0, 1).start()
            before(j, 1, 1).start()

    def sent(src, sem):
        pltpu.make_async_remote_copy(
            src_ref=src, dst_ref=src, send_sem=sem, recv_sem=w_recv.at[0, 0], device_id={"tp": xn}
        ).wait_send()

    def sent_before(j):
        @pl.when(jnp.logical_or(blocks[j] != 3, s < n_seq - 1))
        def _():
            sent(kwin.at[j], before_send.at[j])

    def wait_before(j):
        @pl.when(jnp.logical_or(blocks[j] != 0, s > 0))
        def _():
            for which, win in enumerate((kwin, vwin)):
                pltpu.make_async_remote_copy(
                    src_ref=win.at[j, early],
                    dst_ref=win.at[j, early],
                    send_sem=before_send.at[j],
                    recv_sem=before_recv.at[which, j],
                    device_id={"tp": xn},
                ).wait_recv()

    mine = pl.ds(pl.multiple_of(core * half, half), half)
    theirs = pl.ds(pl.multiple_of((1 - core) * half, half), half)

    def weight(i, stage):
        which = 1 - parity if stage == 3 else parity
        at = cols(2 * i + which, chunk)
        return pltpu.make_async_remote_copy(
            src_ref=(w_hbm if stage == 0 else w_side).at[mine, at],
            dst_ref=w_side.at[mine, at],
            send_sem=w_send.at[stage],
            recv_sem=w_recv.at[min(stage, 2), i],
            device_id=({"tp": xn}, {"seq": plane}, {"seq": peer}, {"seq": peer})[stage],
        )

    def relay_direct(i):
        weight(i, 0).wait_recv()
        weight(i, 1).start()
        weight(i, 2).start()

    def relay_plane(i):
        weight(i, 1).wait_recv()
        weight(i, 3).start()

    for which in range(2):
        early_[which].wait()
        across(which).start()
    tiles = rows // TILE
    for t in range(tiles):
        across_q(t, 0).start()
        across_q(t, 1).start()
    for i in range(FIRST):
        weight(i, 0).start()

    for j in range(2):

        @pl.when(jnp.logical_and(blocks[j] == 0, s == 0))
        def _():
            kwin[j, 0:rows] = jnp.zeros((rows, pair_width), bf16)
            vwin[j, 0:rows] = jnp.zeros((rows, pair_width), bf16)

    def send_halo(urgent):
        @pl.when(x == urgent)
        def _():
            send_before(0)

        @pl.when(x != urgent)
        def _():
            send_before(1)

    @pl.when(ahead)
    def _():
        pl.semaphore_wait(entered, 1)

    across(0).wait_recv()
    across(1).wait_recv()
    send_halo(1)
    for i in range(FIRST, SECOND):
        weight(i, 0).start()
    send_halo(0)

    @pl.loop(SECOND, PAIRS)
    def _(i):
        weight(i, 0).start()

    relay_direct(0)
    for copy in locals_:
        copy.wait()

    causal_q = lax.broadcasted_iota(jnp.int32, (TILE, TILE), 0)
    causal_k = lax.broadcasted_iota(jnp.int32, (TILE, TILE), 1)

    def attend(j, t, quarter):
        row = (s * 4 + blocks[j]) * tiles + t

        def seg_row(at):
            got = seg_ref[pl.ds(jnp.maximum(at, 0), 1), :]
            return jnp.broadcast_to(jnp.where(at >= 0, got, -1), (TILE, TILE))

        if quarter == 0:
            current = seg_row(row)
            down = jnp.transpose(current)
            low, zero = f32(-1e30), f32(0.0)
            bias[:, 0:TILE] = jnp.where(seg_row(row - 2) == down, zero, low)
            bias[:, TILE : 2 * TILE] = jnp.where(seg_row(row - 1) == down, zero, low)
            bias[:, 2 * TILE : 3 * TILE] = jnp.where(
                jnp.logical_and(current == down, causal_k <= causal_q), zero, low
            )
        here = pl.ds(t * TILE, TILE)
        window = pl.ds(t * TILE, 3 * TILE)
        heads = width // HD
        if j == 1 and quarter % 2 == 0:
            across_q(t, quarter // 2).wait_recv()
        for h in range(quarter * (heads // 4), (quarter + 1) * (heads // 4)):
            span = slice(h * HD, (h + 1) * HD)
            kv = slice(h // group * HD, (h // group + 1) * HD)
            scores = lax.dot_general(
                qbuf[j, here, span],
                kwin[j, window, kv],
                (((1,), (1,)), ((), ())),
                preferred_element_type=f32,
            )
            scores = scores * (HD**-0.5) + bias[...]
            weights = jnp.exp(scores - jnp.max(scores, axis=-1, keepdims=True))
            denom = jnp.sum(weights, axis=-1, keepdims=True)
            total = jnp.dot(weights.astype(bf16), vwin[j, window, kv], preferred_element_type=f32)
            att[j, here, span] = (total / denom).astype(bf16)

    def product(j, at, here):
        return jnp.dot(
            att[j, here, cols(x, depth)], w_ref[:, at], preferred_element_type=f32
        ) + jnp.dot(att[j, here, cols(1 - x, depth)], w_side[:, at], preferred_element_type=f32)

    def outward(here, at, group):
        return pltpu.make_async_remote_copy(
            src_ref=part.at[here, at],
            dst_ref=arrived.at[here, at],
            send_sem=out_send.at[0],
            recv_sem=out_recv.at[group],
            device_id={"tp": yn},
        )

    every = pl.ds(0, rows)
    tile0, tile1 = pl.ds(0, TILE), pl.ds(TILE, TILE)

    def whole(i):
        held = w_side.at[theirs, cols(i, pair_cols)]
        pltpu.make_async_remote_copy(
            src_ref=held,
            dst_ref=held,
            send_sem=w_send.at[2],
            recv_sem=w_recv.at[2, i],
            device_id={"seq": peer},
        ).wait_recv()

    def export(i, here, group):
        at = cols(i, pair_cols)
        part[here, at] = product(1, at, here).astype(bf16)
        outward(here, at, group).start()

    def keep(i):
        at = cols(i, 2 * pair_cols)
        own[:, at] = product(0, at, every)

    relay_direct(1)
    relay_plane(0)
    relay_direct(2)
    relay_plane(1)
    wait_before(1)
    attend(1, 0, 0)
    attend(1, 0, 1)
    relay_plane(2)
    relay_direct(3)
    attend(1, 0, 2)
    attend(1, 0, 3)
    whole(0)
    export(0, tile0, 0)
    whole(1)
    export(1, tile0, 0)
    whole(2)
    export(2, tile0, 0)
    relay_direct(4)
    relay_plane(3)
    attend(1, 1, 0)
    whole(3)
    export(3, tile0, 0)
    attend(1, 1, 1)
    relay_plane(4)
    whole(4)
    export(4, tile0, 0)
    relay_direct(5)
    attend(1, 1, 2)
    attend(1, 1, 3)
    relay_direct(6)

    @pl.loop(0, EARLY)
    def _(i):
        export(i, tile1, 0)

    relay_plane(5)
    relay_direct(7)
    whole(5)
    export(5, every, 0)
    wait_before(0)
    attend(0, 0, 0)
    relay_direct(8)
    relay_plane(6)
    attend(0, 0, 1)
    whole(6)
    export(6, every, 0)
    relay_direct(9)
    relay_plane(7)
    attend(0, 0, 2)
    whole(7)
    export(7, every, 0)
    relay_direct(10)
    relay_plane(8)
    attend(0, 0, 3)
    whole(8)
    export(8, every, 0)
    relay_direct(11)
    relay_plane(9)
    attend(0, 1, 0)
    whole(9)
    export(9, every, 0)
    relay_direct(12)
    relay_plane(10)
    attend(0, 1, 1)
    whole(10)
    export(10, every, 0)
    relay_direct(13)
    relay_plane(11)
    attend(0, 1, 2)
    whole(11)
    export(11, every, 0)
    relay_direct(14)
    relay_plane(12)
    attend(0, 1, 3)
    whole(12)
    export(12, every, 0)
    relay_direct(15)
    relay_plane(13)
    keep(0)
    whole(13)
    export(13, every, 0)
    relay_plane(14)
    keep(1)
    whole(14)
    export(14, every, 1)
    relay_plane(15)
    keep(2)
    whole(15)
    export(15, every, 2)

    @pl.loop(3, 8)
    def _(i):
        keep(i)


    sent(kv_out, in_send.at[0])
    sent(qbuf.at[1], in_send.at[1])
    sent_before(0)
    sent_before(1)

    for stage in range(4):
        sent(w_side.at[mine, pl.ds(0, n_out // 2)], w_send.at[stage])

    def settle(at):
        out_ref[:, at] = (own[:, at] + arrived[:, at].astype(f32)).astype(bf16)

    outward(every, pl.ds(0, (PAIRS - 2) * pair_cols), 0).wait_recv()

    @pl.loop(0, PAIRS // 2 - 1)
    def _(i):
        settle(cols(i, 2 * pair_cols))

    for i in range(PAIRS - 2, PAIRS):
        at = cols(i, pair_cols)
        outward(every, at, i - PAIRS + 3).wait_recv()
        settle(at)
    outward(every, pl.ds(0, n_out), 0).wait_send()


def square_shards(n_seq, queries, keys, values, segments, out_weight):
    rows, n_q = queries.shape
    width = n_q // 2
    pair_width = keys.shape[1] // 2
    depth, n_out = out_weight.shape
    bf16 = jnp.bfloat16
    hbm = pl.BlockSpec(memory_space=pltpu.HBM)
    vmem = pl.BlockSpec(memory_space=pltpu.VMEM)
    dma = pltpu.SemaphoreType.DMA
    return pl.pallas_call(
        functools.partial(kernel, n_seq),
        out_shape=jax.ShapeDtypeStruct((rows, n_out), bf16),
        in_specs=[hbm, hbm, hbm, hbm, hbm],
        out_specs=vmem,
        scratch_shapes=[
            pltpu.VMEM((segments.shape[0] // TILE, TILE), jnp.int32),
            pltpu.VMEM((2, rows, pair_width), bf16),
            pltpu.VMEM((2, rows, width), bf16),
            pltpu.VMEM((2, 2 * rows, pair_width), bf16),
            pltpu.VMEM((2, 2 * rows, pair_width), bf16),
            pltpu.VMEM((depth, n_out), bf16),
            pltpu.VMEM((depth, n_out), bf16),
            pltpu.VMEM((2, rows, width), bf16),
            pltpu.VMEM((TILE, 3 * TILE), jnp.float32),
            pltpu.VMEM((rows, n_out), bf16),
            pltpu.VMEM((rows, n_out), jnp.float32),
            pltpu.VMEM((rows, n_out), bf16),
            dma((7,)),
            dma((2,)),
            dma((2 + 2 * rows // TILE,)),
            dma((2,)),
            dma((2, 2)),
            dma((4,)),
            dma((3, PAIRS)),
            dma((1,)),
            dma((3,)),
            pltpu.SemaphoreType.REGULAR,
        ],
        compiler_params=pltpu.CompilerParams(
            collective_id=0, has_side_effects=True, vmem_limit_bytes=50 * 1024 * 1024
        ),
    )(
        *(
            pltpu.with_memory_space_constraint(a, pltpu.HBM)
            for a in (queries, keys, values, segments.reshape(-1, TILE), out_weight)
        )
    )


def solution(mesh):
    placed = (
        P(("seq", "tp"), None),
        P(("seq", "tp"), None),
        P(("seq", "tp"), None),
        P(),
        P("tp", None),
    )
    n_seq, n_tp = mesh.shape["seq"], mesh.shape["tp"]

    def shards(queries, keys, values, segments, out_weight):
        one_head_each = keys.shape[1] == n_tp * HD
        fits = n_tp == 4 and n_seq % 4 == 0 and queries.shape[0] == DOC
        if fits and one_head_each:
            return square_shards(n_seq, queries, keys, values, segments, out_weight)
        return general_shards(queries, keys, values, segments, out_weight)

    return jax.shard_map(
        shards, mesh=mesh, in_specs=placed, out_specs=P(("seq", "tp"), None), check_vma=False
    )
```

```python
import functools

import jax
import jax.numpy as jnp
from jax import lax
from jax.experimental import pallas as pl
from jax.experimental.pallas import tpu as pltpu
from jax.sharding import PartitionSpec as P

KVH = 4
HD = 128
DOC = 256
TILE = DOC // 2


def from_behind(value, axis, steps):
    count = lax.axis_size(axis)
    first, last = (max(0, -steps), min(count, count - steps))
    return lax.ppermute(value, axis, [(source, source + steps) for source in range(first, last)])


def spread_heads(source, copies):
    if copies == 1:
        return source
    rows = source.shape[0]
    widened = jnp.repeat(source.reshape(rows, KVH, HD), copies, axis=1)
    return widened.reshape(rows, KVH * copies * HD)


def general_shards(queries, keys, values, segments, out_weight):
    tp_count = lax.axis_size("tp")
    copies = max(tp_count // KVH, 1)
    tile_rows = DOC // 2
    inverse_root = HD ** (-0.5)
    keys_wide = spread_heads(keys, copies)
    values_wide = spread_heads(values, copies)
    local_queries, local_keys, local_values = (
        lax.all_to_all(queries, "tp", split_axis=1, concat_axis=0, tiled=True),
        lax.all_to_all(keys_wide, "tp", split_axis=1, concat_axis=0, tiled=True),
        lax.all_to_all(values_wide, "tp", split_axis=1, concat_axis=0, tiled=True),
    )
    row_count = local_queries.shape[0]
    kv_local = local_keys.shape[1] // HD
    query_local = local_queries.shape[1] // HD
    local_group = query_local // kv_local
    tile_count = row_count // tile_rows
    first_row = lax.axis_index("seq") * row_count
    closing = jnp.stack([local_keys[row_count - DOC :], local_values[row_count - DOC :]])
    earlier = from_behind(closing, "seq", 1)
    key_ext = jnp.concatenate([earlier[0], local_keys], 0).reshape(row_count + DOC, kv_local, HD)
    value_ext = jnp.concatenate([earlier[1], local_values], 0).reshape(
        row_count + DOC, kv_local, HD
    )
    padded_seg = jnp.concatenate([jnp.full((DOC,), -1, jnp.int32), segments], 0)
    key_seg = lax.dynamic_slice_in_dim(padded_seg, first_row, row_count + DOC)
    query_seg = key_seg[DOC:].reshape(tile_count, tile_rows)
    key_pos = first_row - DOC + jnp.arange(row_count + DOC, dtype=jnp.int32)
    query_pos = (first_row + jnp.arange(row_count, dtype=jnp.int32)).reshape(tile_count, tile_rows)

    def windows(source):
        blocks = source.reshape((tile_count + 2, tile_rows) + source.shape[1:])
        return jnp.concatenate([blocks[:-2], blocks[1:-1], blocks[2:]], 1)

    key_win = windows(key_ext)
    value_win = windows(value_ext)
    pos_win = windows(key_pos)
    seg_win = windows(key_seg)
    query_tiles = local_queries.reshape(tile_count, tile_rows, kv_local, local_group, HD)
    allowed = (pos_win[:, None, :] <= query_pos[:, :, None]) & (
        seg_win[:, None, :] == query_seg[:, :, None]
    )
    allowed = allowed[:, None, None]
    scores = (
        jnp.einsum("ctkgd,cskd->ckgts", query_tiles, key_win, preferred_element_type=jnp.float32)
        * inverse_root
    )
    masked = jnp.where(allowed, scores, jnp.float32(-1e30))
    top_score = jnp.max(masked, axis=-1, keepdims=True)
    weights = jnp.where(allowed, jnp.exp(masked - top_score), jnp.float32(0.0))
    denominator = jnp.sum(weights, axis=-1)
    totals = jnp.einsum(
        "ckgts,cskd->ckgtd",
        weights.astype(jnp.bfloat16),
        value_win,
        preferred_element_type=jnp.float32,
    )
    attended = (totals / denominator[..., None]).astype(jnp.bfloat16)
    attended = jnp.transpose(attended, (0, 3, 1, 2, 4)).reshape(row_count, query_local * HD)
    return lax.psum_scatter(
        jnp.dot(attended, out_weight, preferred_element_type=jnp.float32).astype(jnp.bfloat16),
        "tp",
        scatter_dimension=0,
        tiled=True,
    )


PAIRS = 16
FIRST = 3
SECOND = 5
EARLY = 5


def kernel(
    n_seq,
    q_hbm,
    k_hbm,
    v_hbm,
    seg_hbm,
    w_hbm,
    out_ref,
    seg_ref,
    kv_out,
    qbuf,
    kwin,
    vwin,
    w_ref,
    w_side,
    att,
    bias,
    part,
    own,
    arrived,
    local_sem,
    in_send,
    in_recv,
    before_send,
    before_recv,
    w_send,
    w_recv,
    out_send,
    out_recv,
    entered,
):
    rows, width = qbuf.shape[1], qbuf.shape[2]
    pair_width = kwin.shape[2]
    group = width // pair_width
    depth, n_out = w_ref.shape
    pair_cols = n_out // PAIRS
    chunk = pair_cols // 2
    half = depth // 2
    s = lax.axis_index("seq")
    me = lax.axis_index("tp")
    x = me % 2
    y = me // 2
    xn = y * 2 + 1 - x
    yn = (1 - y) * 2 + x
    core = s % 2
    parity = (s // 2) % 2
    peer = s + 1 - 2 * core
    plane = s + 2 - 4 * parity
    blocks = (me, yn)
    f32, bf16 = jnp.float32, jnp.bfloat16

    def cols(index, size):
        return pl.ds(pl.multiple_of(index * size, size), size)

    late = pl.ds(rows, rows)
    early = pl.ds(0, rows)
    early_ = [
        pltpu.make_async_copy(
            (k_hbm, v_hbm)[which].at[:, cols(1 - y, pair_width)],
            kv_out.at[which],
            local_sem.at[5 + which],
        )
        for which in range(2)
    ]
    for copy in early_:
        copy.start()
    locals_ = [
        pltpu.make_async_copy(k_hbm.at[:, cols(y, pair_width)], kwin.at[0, late], local_sem.at[0]),
        pltpu.make_async_copy(v_hbm.at[:, cols(y, pair_width)], vwin.at[0, late], local_sem.at[1]),
        pltpu.make_async_copy(q_hbm.at[:, cols(y, width)], qbuf.at[0], local_sem.at[2]),
        pltpu.make_async_copy(w_hbm, w_ref, local_sem.at[3]),
        pltpu.make_async_copy(seg_hbm, seg_ref, local_sem.at[4]),
    ]
    for copy in locals_:
        copy.start()

    barrier = pltpu.get_barrier_semaphore()
    for target in ({"tp": xn}, {"tp": yn}, {"seq": peer}, {"seq": plane}):
        pl.semaphore_signal(barrier, inc=1, device_id=target)
    ahead = jnp.logical_and(x == 1, s < n_seq - 1)
    behind = jnp.logical_and(x == 1, s > 0)
    above = jnp.logical_and(ahead, core == 1)
    below = jnp.logical_and(behind, core == 0)

    @pl.when(above)
    def _():
        pl.semaphore_signal(barrier, inc=1, device_id={"seq": s + 1})

    @pl.when(below)
    def _():
        pl.semaphore_signal(barrier, inc=1, device_id={"seq": s - 1})

    pl.semaphore_wait(barrier, 4 + jnp.where(above, 1, 0) + jnp.where(below, 1, 0))

    @pl.when(behind)
    def _():
        pl.semaphore_signal(entered, inc=1, device_id={"seq": s - 1})

    def across(which):
        return pltpu.make_async_remote_copy(
            src_ref=kv_out.at[which],
            dst_ref=(kwin, vwin)[which].at[1, late],
            send_sem=in_send.at[0],
            recv_sem=in_recv.at[which],
            device_id={"tp": yn},
        )

    def across_q(t, g):
        at = pl.ds(t * TILE, TILE)
        part_width = width // 2
        return pltpu.make_async_remote_copy(
            src_ref=q_hbm.at[at, cols((1 - y) * 2 + g, part_width)],
            dst_ref=qbuf.at[1, at, pl.ds(g * part_width, part_width)],
            send_sem=in_send.at[1],
            recv_sem=in_recv.at[2 + 2 * t + g],
            device_id={"tp": yn},
        )

    def before(j, which, hop):
        win = (kwin, vwin)[which]
        src = (k_hbm, v_hbm)[which].at[:, cols(y, pair_width)] if j == 0 else win.at[1, late]
        slot = j + x * (1 - 2 * j)
        return pltpu.make_async_remote_copy(
            src_ref=src,
            dst_ref=win.at[slot, early],
            send_sem=before_send.at[j],
            recv_sem=before_recv.at[which, slot],
            device_id={"seq": lax.rem(s + hop, n_seq), "tp": xn},
        )

    def send_before(j):
        @pl.when(blocks[j] != 3)
        def _():
            before(j, 0, 0).start()
            before(j, 1, 0).start()

        @pl.when(jnp.logical_and(blocks[j] == 3, s < n_seq - 1))
        def _():
            before(j, 0, 1).start()
            before(j, 1, 1).start()

    def sent(src, sem):
        pltpu.make_async_remote_copy(
            src_ref=src, dst_ref=src, send_sem=sem, recv_sem=w_recv.at[0, 0], device_id={"tp": xn}
        ).wait_send()

    def sent_before(j):
        @pl.when(jnp.logical_or(blocks[j] != 3, s < n_seq - 1))
        def _():
            sent(kwin.at[j], before_send.at[j])

    def wait_before(j):
        @pl.when(jnp.logical_or(blocks[j] != 0, s > 0))
        def _():
            for which, win in enumerate((kwin, vwin)):
                pltpu.make_async_remote_copy(
                    src_ref=win.at[j, early],
                    dst_ref=win.at[j, early],
                    send_sem=before_send.at[j],
                    recv_sem=before_recv.at[which, j],
                    device_id={"tp": xn},
                ).wait_recv()

    mine = pl.ds(pl.multiple_of(core * half, half), half)
    theirs = pl.ds(pl.multiple_of((1 - core) * half, half), half)

    def weight(i, stage):
        which = 1 - parity if stage == 3 else parity
        at = cols(2 * i + which, chunk)
        return pltpu.make_async_remote_copy(
            src_ref=(w_hbm if stage == 0 else w_side).at[mine, at],
            dst_ref=w_side.at[mine, at],
            send_sem=w_send.at[stage],
            recv_sem=w_recv.at[min(stage, 2), i],
            device_id=({"tp": xn}, {"seq": plane}, {"seq": peer}, {"seq": peer})[stage],
        )

    def relay_direct(i):
        weight(i, 0).wait_recv()
        weight(i, 1).start()
        weight(i, 2).start()

    def relay_plane(i):
        weight(i, 1).wait_recv()
        weight(i, 3).start()

    for which in range(2):
        early_[which].wait()
        across(which).start()
    tiles = rows // TILE
    for t in range(tiles):
        across_q(t, 0).start()
        across_q(t, 1).start()
    for i in range(FIRST):
        weight(i, 0).start()

    for j in range(2):

        @pl.when(jnp.logical_and(blocks[j] == 0, s == 0))
        def _():
            kwin[j, 0:rows] = jnp.zeros((rows, pair_width), bf16)
            vwin[j, 0:rows] = jnp.zeros((rows, pair_width), bf16)

    def send_halo(urgent):
        @pl.when(x == urgent)
        def _():
            send_before(0)

        @pl.when(x != urgent)
        def _():
            send_before(1)

    @pl.when(ahead)
    def _():
        pl.semaphore_wait(entered, 1)

    across(0).wait_recv()
    across(1).wait_recv()
    send_halo(1)
    for i in range(FIRST, SECOND):
        weight(i, 0).start()
    send_halo(0)

    @pl.loop(SECOND, PAIRS)
    def _(i):
        weight(i, 0).start()

    relay_direct(0)
    for copy in locals_:
        copy.wait()

    causal_q = lax.broadcasted_iota(jnp.int32, (TILE, TILE), 0)
    causal_k = lax.broadcasted_iota(jnp.int32, (TILE, TILE), 1)

    def attend(j, t, quarter):
        row = (s * 4 + blocks[j]) * tiles + t

        def seg_row(at):
            got = seg_ref[pl.ds(jnp.maximum(at, 0), 1), :]
            return jnp.broadcast_to(jnp.where(at >= 0, got, -1), (TILE, TILE))

        if quarter == 0:
            current = seg_row(row)
            down = jnp.transpose(current)
            low, zero = f32(-1e30), f32(0.0)
            bias[:, 0:TILE] = jnp.where(seg_row(row - 2) == down, zero, low)
            bias[:, TILE : 2 * TILE] = jnp.where(seg_row(row - 1) == down, zero, low)
            bias[:, 2 * TILE : 3 * TILE] = jnp.where(
                jnp.logical_and(current == down, causal_k <= causal_q), zero, low
            )
        here = pl.ds(t * TILE, TILE)
        window = pl.ds(t * TILE, 3 * TILE)
        heads = width // HD
        if j == 1 and quarter % 2 == 0:
            across_q(t, quarter // 2).wait_recv()
        for h in range(quarter * (heads // 4), (quarter + 1) * (heads // 4)):
            span = slice(h * HD, (h + 1) * HD)
            kv = slice(h // group * HD, (h // group + 1) * HD)
            scores = lax.dot_general(
                qbuf[j, here, span],
                kwin[j, window, kv],
                (((1,), (1,)), ((), ())),
                preferred_element_type=f32,
            )
            scores = scores * (HD**-0.5) + bias[...]
            weights = jnp.exp(scores - jnp.max(scores, axis=-1, keepdims=True))
            denom = jnp.sum(weights, axis=-1, keepdims=True)
            total = jnp.dot(weights.astype(bf16), vwin[j, window, kv], preferred_element_type=f32)
            att[j, here, span] = (total / denom).astype(bf16)

    def product(j, at, here):
        return jnp.dot(
            att[j, here, cols(x, depth)], w_ref[:, at], preferred_element_type=f32
        ) + jnp.dot(att[j, here, cols(1 - x, depth)], w_side[:, at], preferred_element_type=f32)

    def outward(here, at, group):
        return pltpu.make_async_remote_copy(
            src_ref=part.at[here, at],
            dst_ref=arrived.at[here, at],
            send_sem=out_send.at[0],
            recv_sem=out_recv.at[group],
            device_id={"tp": yn},
        )

    every = pl.ds(0, rows)
    tile0, tile1 = pl.ds(0, TILE), pl.ds(TILE, TILE)

    def whole(i):
        held = w_side.at[theirs, cols(i, pair_cols)]
        pltpu.make_async_remote_copy(
            src_ref=held,
            dst_ref=held,
            send_sem=w_send.at[2],
            recv_sem=w_recv.at[2, i],
            device_id={"seq": peer},
        ).wait_recv()

    def export(i, here, group):
        at = cols(i, pair_cols)
        part[here, at] = product(1, at, here).astype(bf16)
        outward(here, at, group).start()

    def keep(i):
        at = cols(i, 2 * pair_cols)
        own[:, at] = product(0, at, every)

    relay_direct(1)
    relay_plane(0)
    relay_direct(2)
    relay_plane(1)
    wait_before(1)
    attend(1, 0, 0)
    attend(1, 0, 1)
    relay_plane(2)
    relay_direct(3)
    attend(1, 0, 2)
    attend(1, 0, 3)
    whole(0)
    export(0, tile0, 0)
    whole(1)
    export(1, tile0, 0)
    whole(2)
    export(2, tile0, 0)
    relay_direct(4)
    relay_plane(3)
    attend(1, 1, 0)
    whole(3)
    export(3, tile0, 0)
    attend(1, 1, 1)
    relay_plane(4)
    whole(4)
    export(4, tile0, 0)
    relay_direct(5)
    attend(1, 1, 2)
    attend(1, 1, 3)
    relay_direct(6)

    @pl.loop(0, EARLY)
    def _(i):
        export(i, tile1, 0)

    relay_plane(5)
    relay_direct(7)
    whole(5)
    export(5, every, 0)
    wait_before(0)
    attend(0, 0, 0)
    relay_direct(8)
    relay_plane(6)
    attend(0, 0, 1)
    whole(6)
    export(6, every, 0)
    relay_direct(9)
    relay_plane(7)
    attend(0, 0, 2)
    whole(7)
    export(7, every, 0)
    relay_direct(10)
    relay_plane(8)
    attend(0, 0, 3)
    whole(8)
    export(8, every, 0)
    relay_direct(11)
    relay_plane(9)
    attend(0, 1, 0)
    whole(9)
    export(9, every, 0)
    relay_direct(12)
    relay_plane(10)
    attend(0, 1, 1)
    whole(10)
    export(10, every, 0)
    relay_direct(13)
    relay_plane(11)
    attend(0, 1, 2)
    whole(11)
    export(11, every, 0)
    relay_direct(14)
    relay_plane(12)
    attend(0, 1, 3)
    whole(12)
    export(12, every, 0)
    relay_direct(15)
    relay_plane(13)
    keep(0)
    whole(13)
    export(13, every, 0)
    relay_plane(14)
    keep(1)
    whole(14)

    @pl.when(core == 0)
    def _():
        export(14, every, 1)

    relay_plane(15)
    keep(2)
    whole(15)

    @pl.when(core == 0)
    def _():
        export(15, every, 2)

    keep(3)

    @pl.when(core == 1)
    def _():
        export(14, every, 1)


    @pl.loop(4, 6)
    def _(i):
        keep(i)


    @pl.when(core == 1)
    def _():
        export(15, every, 2)


    @pl.loop(6, 8)
    def _(i):
        keep(i)


    sent(kv_out, in_send.at[0])
    sent(qbuf.at[1], in_send.at[1])
    sent_before(0)
    sent_before(1)

    for stage in range(4):
        sent(w_side.at[mine, pl.ds(0, n_out // 2)], w_send.at[stage])

    def settle(at):
        out_ref[:, at] = (own[:, at] + arrived[:, at].astype(f32)).astype(bf16)

    outward(every, pl.ds(0, (PAIRS - 2) * pair_cols), 0).wait_recv()

    @pl.loop(0, PAIRS // 2 - 1)
    def _(i):
        settle(cols(i, 2 * pair_cols))

    for i in range(PAIRS - 2, PAIRS):
        at = cols(i, pair_cols)
        outward(every, at, i - PAIRS + 3).wait_recv()
        settle(at)
    outward(every, pl.ds(0, n_out), 0).wait_send()


def square_shards(n_seq, queries, keys, values, segments, out_weight):
    rows, n_q = queries.shape
    width = n_q // 2
    pair_width = keys.shape[1] // 2
    depth, n_out = out_weight.shape
    bf16 = jnp.bfloat16
    hbm = pl.BlockSpec(memory_space=pltpu.HBM)
    vmem = pl.BlockSpec(memory_space=pltpu.VMEM)
    dma = pltpu.SemaphoreType.DMA
    return pl.pallas_call(
        functools.partial(kernel, n_seq),
        out_shape=jax.ShapeDtypeStruct((rows, n_out), bf16),
        in_specs=[hbm, hbm, hbm, hbm, hbm],
        out_specs=vmem,
        scratch_shapes=[
            pltpu.VMEM((segments.shape[0] // TILE, TILE), jnp.int32),
            pltpu.VMEM((2, rows, pair_width), bf16),
            pltpu.VMEM((2, rows, width), bf16),
            pltpu.VMEM((2, 2 * rows, pair_width), bf16),
            pltpu.VMEM((2, 2 * rows, pair_width), bf16),
            pltpu.VMEM((depth, n_out), bf16),
            pltpu.VMEM((depth, n_out), bf16),
            pltpu.VMEM((2, rows, width), bf16),
            pltpu.VMEM((TILE, 3 * TILE), jnp.float32),
            pltpu.VMEM((rows, n_out), bf16),
            pltpu.VMEM((rows, n_out), jnp.float32),
            pltpu.VMEM((rows, n_out), bf16),
            dma((7,)),
            dma((2,)),
            dma((2 + 2 * rows // TILE,)),
            dma((2,)),
            dma((2, 2)),
            dma((4,)),
            dma((3, PAIRS)),
            dma((1,)),
            dma((3,)),
            pltpu.SemaphoreType.REGULAR,
        ],
        compiler_params=pltpu.CompilerParams(
            collective_id=0, has_side_effects=True, vmem_limit_bytes=50 * 1024 * 1024
        ),
    )(
        *(
            pltpu.with_memory_space_constraint(a, pltpu.HBM)
            for a in (queries, keys, values, segments.reshape(-1, TILE), out_weight)
        )
    )


def solution(mesh):
    placed = (
        P(("seq", "tp"), None),
        P(("seq", "tp"), None),
        P(("seq", "tp"), None),
        P(),
        P("tp", None),
    )
    n_seq, n_tp = mesh.shape["seq"], mesh.shape["tp"]

    def shards(queries, keys, values, segments, out_weight):
        one_head_each = keys.shape[1] == n_tp * HD
        fits = n_tp == 4 and n_seq % 4 == 0 and queries.shape[0] == DOC
        if fits and one_head_each:
            return square_shards(n_seq, queries, keys, values, segments, out_weight)
        return general_shards(queries, keys, values, segments, out_weight)

    return jax.shard_map(
        shards, mesh=mesh, in_specs=placed, out_specs=P(("seq", "tp"), None), check_vma=False
    )
```

```python
import functools

import jax
import jax.numpy as jnp
from jax import lax
from jax.experimental import pallas as pl
from jax.experimental.pallas import tpu as pltpu
from jax.sharding import PartitionSpec as P

KVH = 4
HD = 128
DOC = 256
TILE = DOC // 2


def from_behind(value, axis, steps):
    count = lax.axis_size(axis)
    first, last = (max(0, -steps), min(count, count - steps))
    return lax.ppermute(value, axis, [(source, source + steps) for source in range(first, last)])


def spread_heads(source, copies):
    if copies == 1:
        return source
    rows = source.shape[0]
    widened = jnp.repeat(source.reshape(rows, KVH, HD), copies, axis=1)
    return widened.reshape(rows, KVH * copies * HD)


def general_shards(queries, keys, values, segments, out_weight):
    tp_count = lax.axis_size("tp")
    copies = max(tp_count // KVH, 1)
    tile_rows = DOC // 2
    inverse_root = HD ** (-0.5)
    keys_wide = spread_heads(keys, copies)
    values_wide = spread_heads(values, copies)
    local_queries, local_keys, local_values = (
        lax.all_to_all(queries, "tp", split_axis=1, concat_axis=0, tiled=True),
        lax.all_to_all(keys_wide, "tp", split_axis=1, concat_axis=0, tiled=True),
        lax.all_to_all(values_wide, "tp", split_axis=1, concat_axis=0, tiled=True),
    )
    row_count = local_queries.shape[0]
    kv_local = local_keys.shape[1] // HD
    query_local = local_queries.shape[1] // HD
    local_group = query_local // kv_local
    tile_count = row_count // tile_rows
    first_row = lax.axis_index("seq") * row_count
    closing = jnp.stack([local_keys[row_count - DOC :], local_values[row_count - DOC :]])
    earlier = from_behind(closing, "seq", 1)
    key_ext = jnp.concatenate([earlier[0], local_keys], 0).reshape(row_count + DOC, kv_local, HD)
    value_ext = jnp.concatenate([earlier[1], local_values], 0).reshape(
        row_count + DOC, kv_local, HD
    )
    padded_seg = jnp.concatenate([jnp.full((DOC,), -1, jnp.int32), segments], 0)
    key_seg = lax.dynamic_slice_in_dim(padded_seg, first_row, row_count + DOC)
    query_seg = key_seg[DOC:].reshape(tile_count, tile_rows)
    key_pos = first_row - DOC + jnp.arange(row_count + DOC, dtype=jnp.int32)
    query_pos = (first_row + jnp.arange(row_count, dtype=jnp.int32)).reshape(tile_count, tile_rows)

    def windows(source):
        blocks = source.reshape((tile_count + 2, tile_rows) + source.shape[1:])
        return jnp.concatenate([blocks[:-2], blocks[1:-1], blocks[2:]], 1)

    key_win = windows(key_ext)
    value_win = windows(value_ext)
    pos_win = windows(key_pos)
    seg_win = windows(key_seg)
    query_tiles = local_queries.reshape(tile_count, tile_rows, kv_local, local_group, HD)
    allowed = (pos_win[:, None, :] <= query_pos[:, :, None]) & (
        seg_win[:, None, :] == query_seg[:, :, None]
    )
    allowed = allowed[:, None, None]
    scores = (
        jnp.einsum("ctkgd,cskd->ckgts", query_tiles, key_win, preferred_element_type=jnp.float32)
        * inverse_root
    )
    masked = jnp.where(allowed, scores, jnp.float32(-1e30))
    top_score = jnp.max(masked, axis=-1, keepdims=True)
    weights = jnp.where(allowed, jnp.exp(masked - top_score), jnp.float32(0.0))
    denominator = jnp.sum(weights, axis=-1)
    totals = jnp.einsum(
        "ckgts,cskd->ckgtd",
        weights.astype(jnp.bfloat16),
        value_win,
        preferred_element_type=jnp.float32,
    )
    attended = (totals / denominator[..., None]).astype(jnp.bfloat16)
    attended = jnp.transpose(attended, (0, 3, 1, 2, 4)).reshape(row_count, query_local * HD)
    return lax.psum_scatter(
        jnp.dot(attended, out_weight, preferred_element_type=jnp.float32).astype(jnp.bfloat16),
        "tp",
        scatter_dimension=0,
        tiled=True,
    )


PAIRS = 16
FIRST = 3
SECOND = 5
EARLY = 5


def kernel(
    n_seq,
    q_hbm,
    k_hbm,
    v_hbm,
    seg_hbm,
    w_hbm,
    out_ref,
    seg_ref,
    kv_out,
    qbuf,
    kwin,
    vwin,
    w_ref,
    w_side,
    att,
    bias,
    part,
    own,
    arrived,
    local_sem,
    in_send,
    in_recv,
    before_send,
    before_recv,
    w_send,
    w_recv,
    out_send,
    out_recv,
    entered,
):
    rows, width = qbuf.shape[1], qbuf.shape[2]
    pair_width = kwin.shape[2]
    group = width // pair_width
    depth, n_out = w_ref.shape
    pair_cols = n_out // PAIRS
    chunk = pair_cols // 2
    half = depth // 2
    s = lax.axis_index("seq")
    me = lax.axis_index("tp")
    x = me % 2
    y = me // 2
    xn = y * 2 + 1 - x
    yn = (1 - y) * 2 + x
    core = s % 2
    parity = (s // 2) % 2
    peer = s + 1 - 2 * core
    plane = s + 2 - 4 * parity
    blocks = (me, yn)
    f32, bf16 = jnp.float32, jnp.bfloat16

    def cols(index, size):
        return pl.ds(pl.multiple_of(index * size, size), size)

    late = pl.ds(rows, rows)
    early = pl.ds(0, rows)
    barrier = pltpu.get_barrier_semaphore()
    for target in ({"tp": yn}, {"tp": xn}, {"seq": plane}, {"seq": peer}):
        pl.semaphore_signal(barrier, inc=1, device_id=target)
    ahead = jnp.logical_and(x == 1, s < n_seq - 1)
    behind = jnp.logical_and(x == 1, s > 0)
    above = jnp.logical_and(ahead, core == 1)
    below = jnp.logical_and(behind, core == 0)

    @pl.when(above)
    def _():
        pl.semaphore_signal(barrier, inc=1, device_id={"seq": s + 1})

    @pl.when(below)
    def _():
        pl.semaphore_signal(barrier, inc=1, device_id={"seq": s - 1})

    early_ = [
        pltpu.make_async_copy(
            (k_hbm, v_hbm)[which].at[:, cols(1 - y, pair_width)],
            kv_out.at[which],
            local_sem.at[5 + which],
        )
        for which in range(2)
    ]
    for copy in early_:
        copy.start()
    locals_ = [
        pltpu.make_async_copy(k_hbm.at[:, cols(y, pair_width)], kwin.at[0, late], local_sem.at[0]),
        pltpu.make_async_copy(v_hbm.at[:, cols(y, pair_width)], vwin.at[0, late], local_sem.at[1]),
        pltpu.make_async_copy(q_hbm.at[:, cols(y, width)], qbuf.at[0], local_sem.at[2]),
        pltpu.make_async_copy(w_hbm, w_ref, local_sem.at[3]),
        pltpu.make_async_copy(seg_hbm, seg_ref, local_sem.at[4]),
    ]
    for copy in locals_:
        copy.start()

    pl.semaphore_wait(barrier, 4 + jnp.where(above, 1, 0) + jnp.where(below, 1, 0))

    @pl.when(behind)
    def _():
        pl.semaphore_signal(entered, inc=1, device_id={"seq": s - 1})

    def across(which):
        return pltpu.make_async_remote_copy(
            src_ref=kv_out.at[which],
            dst_ref=(kwin, vwin)[which].at[1, late],
            send_sem=in_send.at[0],
            recv_sem=in_recv.at[which],
            device_id={"tp": yn},
        )

    def across_q(t, g):
        at = pl.ds(t * TILE, TILE)
        part_width = width // 2
        return pltpu.make_async_remote_copy(
            src_ref=q_hbm.at[at, cols((1 - y) * 2 + g, part_width)],
            dst_ref=qbuf.at[1, at, pl.ds(g * part_width, part_width)],
            send_sem=in_send.at[1],
            recv_sem=in_recv.at[2 + 2 * t + g],
            device_id={"tp": yn},
        )

    def before(j, which, hop):
        win = (kwin, vwin)[which]
        src = (k_hbm, v_hbm)[which].at[:, cols(y, pair_width)] if j == 0 else win.at[1, late]
        slot = j + x * (1 - 2 * j)
        return pltpu.make_async_remote_copy(
            src_ref=src,
            dst_ref=win.at[slot, early],
            send_sem=before_send.at[j],
            recv_sem=before_recv.at[which, slot],
            device_id={"seq": lax.rem(s + hop, n_seq), "tp": xn},
        )

    def send_before(j):
        @pl.when(blocks[j] != 3)
        def _():
            before(j, 0, 0).start()
            before(j, 1, 0).start()

        @pl.when(jnp.logical_and(blocks[j] == 3, s < n_seq - 1))
        def _():
            before(j, 0, 1).start()
            before(j, 1, 1).start()

    def sent(src, sem):
        pltpu.make_async_remote_copy(
            src_ref=src, dst_ref=src, send_sem=sem, recv_sem=w_recv.at[0, 0], device_id={"tp": xn}
        ).wait_send()

    def sent_before(j):
        @pl.when(jnp.logical_or(blocks[j] != 3, s < n_seq - 1))
        def _():
            sent(kwin.at[j], before_send.at[j])

    def wait_before(j):
        @pl.when(jnp.logical_or(blocks[j] != 0, s > 0))
        def _():
            for which, win in enumerate((kwin, vwin)):
                pltpu.make_async_remote_copy(
                    src_ref=win.at[j, early],
                    dst_ref=win.at[j, early],
                    send_sem=before_send.at[j],
                    recv_sem=before_recv.at[which, j],
                    device_id={"tp": xn},
                ).wait_recv()

    mine = pl.ds(pl.multiple_of(core * half, half), half)
    theirs = pl.ds(pl.multiple_of((1 - core) * half, half), half)

    def weight(i, stage):
        which = 1 - parity if stage == 3 else parity
        at = cols(2 * i + which, chunk)
        return pltpu.make_async_remote_copy(
            src_ref=(w_hbm if stage == 0 else w_side).at[mine, at],
            dst_ref=w_side.at[mine, at],
            send_sem=w_send.at[stage],
            recv_sem=w_recv.at[min(stage, 2), i],
            device_id=({"tp": xn}, {"seq": plane}, {"seq": peer}, {"seq": peer})[stage],
        )

    def relay_direct(i):
        weight(i, 0).wait_recv()
        weight(i, 1).start()
        weight(i, 2).start()

    def relay_plane(i):
        weight(i, 1).wait_recv()
        weight(i, 3).start()

    for which in range(2):
        early_[which].wait()
        across(which).start()
    tiles = rows // TILE
    for t in range(tiles):
        across_q(t, 0).start()
        across_q(t, 1).start()
    for i in range(FIRST):
        weight(i, 0).start()

    for j in range(2):

        @pl.when(jnp.logical_and(blocks[j] == 0, s == 0))
        def _():
            kwin[j, 0:rows] = jnp.zeros((rows, pair_width), bf16)
            vwin[j, 0:rows] = jnp.zeros((rows, pair_width), bf16)

    def send_halo(urgent):
        @pl.when(x == urgent)
        def _():
            send_before(0)

        @pl.when(x != urgent)
        def _():
            send_before(1)

    @pl.when(ahead)
    def _():
        pl.semaphore_wait(entered, 1)

    across(0).wait_recv()
    across(1).wait_recv()
    send_halo(1)
    for i in range(FIRST, SECOND):
        weight(i, 0).start()
    send_halo(0)

    @pl.loop(SECOND, PAIRS)
    def _(i):
        weight(i, 0).start()

    relay_direct(0)
    for copy in locals_:
        copy.wait()

    causal_q = lax.broadcasted_iota(jnp.int32, (TILE, TILE), 0)
    causal_k = lax.broadcasted_iota(jnp.int32, (TILE, TILE), 1)

    def attend(j, t, quarter):
        row = (s * 4 + blocks[j]) * tiles + t

        def seg_row(at):
            got = seg_ref[pl.ds(jnp.maximum(at, 0), 1), :]
            return jnp.broadcast_to(jnp.where(at >= 0, got, -1), (TILE, TILE))

        if quarter == 0:
            current = seg_row(row)
            down = jnp.transpose(current)
            low, zero = f32(-1e30), f32(0.0)
            bias[:, 0:TILE] = jnp.where(seg_row(row - 2) == down, zero, low)
            bias[:, TILE : 2 * TILE] = jnp.where(seg_row(row - 1) == down, zero, low)
            bias[:, 2 * TILE : 3 * TILE] = jnp.where(
                jnp.logical_and(current == down, causal_k <= causal_q), zero, low
            )
        here = pl.ds(t * TILE, TILE)
        window = pl.ds(t * TILE, 3 * TILE)
        heads = width // HD
        if j == 1 and quarter % 2 == 0:
            across_q(t, quarter // 2).wait_recv()
        for h in range(quarter * (heads // 4), (quarter + 1) * (heads // 4)):
            span = slice(h * HD, (h + 1) * HD)
            kv = slice(h // group * HD, (h // group + 1) * HD)
            scores = lax.dot_general(
                qbuf[j, here, span],
                kwin[j, window, kv],
                (((1,), (1,)), ((), ())),
                preferred_element_type=f32,
            )
            scores = scores * (HD**-0.5) + bias[...]
            weights = jnp.exp(scores - jnp.max(scores, axis=-1, keepdims=True))
            denom = jnp.sum(weights, axis=-1, keepdims=True)
            total = jnp.dot(weights.astype(bf16), vwin[j, window, kv], preferred_element_type=f32)
            att[j, here, span] = (total / denom).astype(bf16)

    def product(j, at, here):
        return jnp.dot(
            att[j, here, cols(x, depth)], w_ref[:, at], preferred_element_type=f32
        ) + jnp.dot(att[j, here, cols(1 - x, depth)], w_side[:, at], preferred_element_type=f32)

    def outward(here, at, group):
        return pltpu.make_async_remote_copy(
            src_ref=part.at[here, at],
            dst_ref=arrived.at[here, at],
            send_sem=out_send.at[0],
            recv_sem=out_recv.at[group],
            device_id={"tp": yn},
        )

    every = pl.ds(0, rows)
    tile0, tile1 = pl.ds(0, TILE), pl.ds(TILE, TILE)

    def whole(i):
        held = w_side.at[theirs, cols(i, pair_cols)]
        pltpu.make_async_remote_copy(
            src_ref=held,
            dst_ref=held,
            send_sem=w_send.at[2],
            recv_sem=w_recv.at[2, i],
            device_id={"seq": peer},
        ).wait_recv()

    def export(i, here, group):
        at = cols(i, pair_cols)
        part[here, at] = product(1, at, here).astype(bf16)
        outward(here, at, group).start()

    def keep(i):
        at = cols(i, 2 * pair_cols)
        own[:, at] = product(0, at, every)

    relay_direct(1)
    relay_plane(0)
    relay_direct(2)
    relay_plane(1)
    wait_before(1)
    attend(1, 0, 0)
    attend(1, 0, 1)
    relay_plane(2)
    relay_direct(3)
    attend(1, 0, 2)
    attend(1, 0, 3)
    whole(0)
    export(0, tile0, 0)
    whole(1)
    export(1, tile0, 0)
    whole(2)
    export(2, tile0, 0)
    relay_direct(4)
    relay_plane(3)
    attend(1, 1, 0)
    whole(3)
    export(3, tile0, 0)
    attend(1, 1, 1)
    relay_plane(4)
    whole(4)
    export(4, tile0, 0)
    relay_direct(5)
    attend(1, 1, 2)
    attend(1, 1, 3)
    relay_direct(6)

    @pl.loop(0, EARLY)
    def _(i):
        export(i, tile1, 0)

    relay_plane(5)
    relay_direct(7)
    whole(5)
    export(5, every, 0)
    wait_before(0)
    attend(0, 0, 0)
    relay_direct(8)
    relay_plane(6)
    attend(0, 0, 1)
    whole(6)
    export(6, every, 0)
    relay_direct(9)
    relay_plane(7)
    attend(0, 0, 2)
    whole(7)
    export(7, every, 0)
    relay_direct(10)
    relay_plane(8)
    attend(0, 0, 3)
    whole(8)
    export(8, every, 0)
    relay_direct(11)
    relay_plane(9)
    attend(0, 1, 0)
    whole(9)
    export(9, every, 0)
    relay_direct(12)
    relay_plane(10)
    attend(0, 1, 1)
    whole(10)
    export(10, every, 0)
    relay_direct(13)
    relay_plane(11)
    attend(0, 1, 2)
    whole(11)
    export(11, every, 0)
    relay_direct(14)
    relay_plane(12)
    attend(0, 1, 3)
    whole(12)
    export(12, every, 0)
    relay_direct(15)
    relay_plane(13)
    keep(0)
    whole(13)
    export(13, every, 0)
    relay_plane(14)
    keep(1)
    whole(14)

    @pl.when(core == 0)
    def _():
        export(14, every, 1)

    relay_plane(15)
    keep(2)
    whole(15)

    @pl.when(core == 0)
    def _():
        export(15, every, 2)

    keep(3)

    @pl.when(core == 1)
    def _():
        export(14, every, 1)


    @pl.loop(4, 6)
    def _(i):
        keep(i)


    @pl.when(core == 1)
    def _():
        export(15, every, 2)


    @pl.loop(6, 8)
    def _(i):
        keep(i)


    sent(kv_out, in_send.at[0])
    sent(qbuf.at[1], in_send.at[1])
    sent_before(0)
    sent_before(1)

    for stage in range(4):
        sent(w_side.at[mine, pl.ds(0, n_out // 2)], w_send.at[stage])

    def settle(at):
        out_ref[:, at] = (own[:, at] + arrived[:, at].astype(f32)).astype(bf16)

    outward(every, pl.ds(0, (PAIRS - 2) * pair_cols), 0).wait_recv()

    @pl.loop(0, PAIRS // 2 - 1)
    def _(i):
        settle(cols(i, 2 * pair_cols))

    for i in range(PAIRS - 2, PAIRS):
        at = cols(i, pair_cols)
        outward(every, at, i - PAIRS + 3).wait_recv()
        settle(at)
    outward(every, pl.ds(0, n_out), 0).wait_send()


def square_shards(n_seq, queries, keys, values, segments, out_weight):
    rows, n_q = queries.shape
    width = n_q // 2
    pair_width = keys.shape[1] // 2
    depth, n_out = out_weight.shape
    bf16 = jnp.bfloat16
    hbm = pl.BlockSpec(memory_space=pltpu.HBM)
    vmem = pl.BlockSpec(memory_space=pltpu.VMEM)
    dma = pltpu.SemaphoreType.DMA
    return pl.pallas_call(
        functools.partial(kernel, n_seq),
        out_shape=jax.ShapeDtypeStruct((rows, n_out), bf16),
        in_specs=[hbm, hbm, hbm, hbm, hbm],
        out_specs=vmem,
        scratch_shapes=[
            pltpu.VMEM((segments.shape[0] // TILE, TILE), jnp.int32),
            pltpu.VMEM((2, rows, pair_width), bf16),
            pltpu.VMEM((2, rows, width), bf16),
            pltpu.VMEM((2, 2 * rows, pair_width), bf16),
            pltpu.VMEM((2, 2 * rows, pair_width), bf16),
            pltpu.VMEM((depth, n_out), bf16),
            pltpu.VMEM((depth, n_out), bf16),
            pltpu.VMEM((2, rows, width), bf16),
            pltpu.VMEM((TILE, 3 * TILE), jnp.float32),
            pltpu.VMEM((rows, n_out), bf16),
            pltpu.VMEM((rows, n_out), jnp.float32),
            pltpu.VMEM((rows, n_out), bf16),
            dma((7,)),
            dma((2,)),
            dma((2 + 2 * rows // TILE,)),
            dma((2,)),
            dma((2, 2)),
            dma((4,)),
            dma((3, PAIRS)),
            dma((1,)),
            dma((3,)),
            pltpu.SemaphoreType.REGULAR,
        ],
        compiler_params=pltpu.CompilerParams(
            collective_id=0, has_side_effects=True, vmem_limit_bytes=50 * 1024 * 1024
        ),
    )(
        *(
            pltpu.with_memory_space_constraint(a, pltpu.HBM)
            for a in (queries, keys, values, segments.reshape(-1, TILE), out_weight)
        )
    )


def solution(mesh):
    placed = (
        P(("seq", "tp"), None),
        P(("seq", "tp"), None),
        P(("seq", "tp"), None),
        P(),
        P("tp", None),
    )
    n_seq, n_tp = mesh.shape["seq"], mesh.shape["tp"]

    def shards(queries, keys, values, segments, out_weight):
        one_head_each = keys.shape[1] == n_tp * HD
        fits = n_tp == 4 and n_seq % 4 == 0 and queries.shape[0] == DOC
        if fits and one_head_each:
            return square_shards(n_seq, queries, keys, values, segments, out_weight)
        return general_shards(queries, keys, values, segments, out_weight)

    return jax.shard_map(
        shards, mesh=mesh, in_specs=placed, out_specs=P(("seq", "tp"), None), check_vma=False
    )
```
